32 devices in a mesh: dp: 1 (over z), tp: 4 (over y), cp: 8 (over x, core).
Axes of the slice: x: 4, y: 4, z: 1, core: 2. Of those that a mesh axis runs over, the one named last changes fastest.
The devices are a block of a 4x4x8 slice.
Arguments:
- x: bfloat16 [2048, 3584], P(('dp', 'cp'))
- doc_id: int32 [2048], P(('dp', 'cp'))
- pos_in_doc: int32 [2048], P(('dp', 'cp'))
- norm_gain: float32 [3584], replicated
- w_q: bfloat16 [3584, 3584], P(None, 'tp')
- w_k: bfloat16 [3584, 512], P(None, 'tp')
- w_v: bfloat16 [3584, 512], P(None, 'tp')
- w_o: bfloat16 [3584, 3584], P('tp')
- inv_freq: float32 [64], replicated
Outputs:
- output 1: bfloat16 [2048, 3584], P(('dp', 'cp'))
- output 2: bfloat16 [2048, 4, 128], P(('dp', 'cp'), 'tp')
- output 3: bfloat16 [2048, 4, 128], P(('dp', 'cp'), 'tp')
All inputs are finite; a program needn't handle non-finite values.
Results may differ from the reference program's by a relative error of at most 0.00168.
Values are sent between devices in bfloat16 or wider.
A program may use at most 768 MiB of HBM per device.

```python
import jax
import jax.numpy as jnp
from jax import lax

TOKENS = 2048
CP_SIZE = 8
D_MODEL = 3584
Q_HEADS = 28
KV_HEADS = 4
HEAD_DIM = 128
DOC_LEN = 96
ROPE_THETA = 1000000
QUERY_ROWS = 128

PIECE_LEN = TOKENS // (2 * CP_SIZE)
GROUP_SIZE = Q_HEADS // KV_HEADS
MAX_DOCS = TOKENS // (DOC_LEN // 2) + 2


def to_stored(glob_arr):
    pieces = glob_arr.reshape((2 * CP_SIZE, PIECE_LEN) + glob_arr.shape[1:])
    paired = jnp.stack([pieces[:CP_SIZE], pieces[CP_SIZE:][::-1]], axis=1)
    return paired.reshape(glob_arr.shape)


def draw_documents(doc_key):
    key_long, key_before, key_after = jax.random.split(doc_key, 3)
    first_piece = (DOC_LEN - 2) // PIECE_LEN + 1
    long_piece = jax.random.randint(key_long, (), first_piece, 2 * CP_SIZE)
    long_start = long_piece * PIECE_LEN - DOC_LEN + 1
    long_end = long_start + DOC_LEN
    lens_before = jax.random.randint(key_before, (MAX_DOCS,), DOC_LEN // 2, DOC_LEN + 1)
    lens_after = jax.random.randint(key_after, (MAX_DOCS,), DOC_LEN // 2, DOC_LEN + 1)
    starts_before = jnp.cumsum(lens_before)
    starts_after = long_end + jnp.cumsum(lens_after) - lens_after
    start_marks = jnp.zeros((TOKENS,), jnp.int32).at[0].set(1).at[long_start].set(1)
    start_marks = start_marks.at[jnp.where(starts_before < long_start, starts_before, TOKENS)].set(1, mode='drop')
    start_marks = start_marks.at[starts_after].set(1, mode='drop')
    doc_glob = jnp.cumsum(start_marks) - 1
    tok_index = jnp.arange(TOKENS)
    pos_glob = tok_index - lax.cummax(tok_index * start_marks, axis=0)
    return doc_glob.astype(jnp.int32), pos_glob.astype(jnp.int32)


def normal_weight(weight_key, fan_in, fan_out):
    return (jax.random.normal(weight_key, (fan_in, fan_out), jnp.float32) * fan_in ** -0.5).astype(jnp.bfloat16)


def setup_inputs(seed: int = 0, part: int = 0) -> dict:
    part_key = jax.random.fold_in(jax.random.key(seed), part)
    key_doc, key_noise, key_drift = jax.random.split(part_key, 3)
    shared = jax.random.split(jax.random.key(seed + 1), 6)
    doc_glob, pos_glob = draw_documents(key_doc)
    pos_ratio = pos_glob.astype(jnp.float32) / DOC_LEN
    drift_dir = jax.random.normal(key_drift, (D_MODEL,), jnp.float32)
    x_noise = jax.random.normal(key_noise, (TOKENS, D_MODEL), jnp.float32)
    x_glob = x_noise + 3.0 * pos_ratio[:, None] * drift_dir[None, :]
    norm_gain = 1.0 + 0.25 * jax.random.normal(shared[0], (D_MODEL,), jnp.float32)
    w_q = normal_weight(shared[1], D_MODEL, Q_HEADS * HEAD_DIM)
    w_k = normal_weight(shared[2], D_MODEL, KV_HEADS * HEAD_DIM)
    w_v = normal_weight(shared[3], D_MODEL, KV_HEADS * HEAD_DIM)
    w_o = normal_weight(shared[4], Q_HEADS * HEAD_DIM, D_MODEL)
    base_freq = ROPE_THETA ** (-jnp.arange(0, HEAD_DIM, 2, dtype=jnp.float32) / HEAD_DIM)
    inv_freq = base_freq * jnp.exp(0.1 * jax.random.normal(shared[5], (HEAD_DIM // 2,), jnp.float32))
    return {'x': to_stored(x_glob).astype(jnp.bfloat16), 'doc_id': to_stored(doc_glob), 'pos_in_doc': to_stored(pos_glob), 'norm_gain': norm_gain, 'w_q': w_q, 'w_k': w_k, 'w_v': w_v, 'w_o': w_o, 'inv_freq': inv_freq}


def apply_rope(vectors, cos_t, sin_t):
    half_dim = vectors.shape[-1] // 2
    lower_half = vectors[..., :half_dim].astype(jnp.float32)
    upper_half = vectors[..., half_dim:].astype(jnp.float32)
    turned = jnp.concatenate([lower_half * cos_t - upper_half * sin_t, upper_half * cos_t + lower_half * sin_t], axis=-1)
    return turned.astype(jnp.bfloat16)


def reference(x, doc_id, pos_in_doc, norm_gain, w_q, w_k, w_v, w_o, inv_freq):
    x_f32 = x.astype(jnp.float32)
    inv_rms = lax.rsqrt(jnp.mean(x_f32 * x_f32, axis=-1, keepdims=True) + 1e-5)
    normed = (x_f32 * inv_rms * norm_gain).astype(jnp.bfloat16)
    q_new = jnp.dot(normed, w_q, preferred_element_type=jnp.float32).astype(jnp.bfloat16).reshape(TOKENS, KV_HEADS, GROUP_SIZE, HEAD_DIM)
    k_new = jnp.dot(normed, w_k, preferred_element_type=jnp.float32).astype(jnp.bfloat16).reshape(TOKENS, KV_HEADS, HEAD_DIM)
    v_new = jnp.dot(normed, w_v, preferred_element_type=jnp.float32).astype(jnp.bfloat16).reshape(TOKENS, KV_HEADS, HEAD_DIM)
    rope_angle = pos_in_doc.astype(jnp.float32)[:, None] * inv_freq[None, :]
    cos_t = jnp.cos(rope_angle)
    sin_t = jnp.sin(rope_angle)
    q_rot = apply_rope(q_new, cos_t[:, None, None, :], sin_t[:, None, None, :])
    k_rot = apply_rope(k_new, cos_t[:, None, :], sin_t[:, None, :])
    tok_index = to_stored(jnp.arange(TOKENS))
    k_f32 = k_rot.astype(jnp.float32)
    v_f32 = v_new.astype(jnp.float32)
    blocks = TOKENS // QUERY_ROWS

    def attend(block_args):
        q_blk, doc_blk, idx_blk = block_args
        scores = jnp.einsum('qngd,knd->ngqk', q_blk.astype(jnp.float32), k_f32) * (HEAD_DIM ** -0.5)
        visible = (doc_blk[:, None] == doc_id[None, :]) & (tok_index[None, :] <= idx_blk[:, None])
        scores = jnp.where(visible, scores, -1e30)
        attn_probs = jax.nn.softmax(scores, axis=-1).astype(jnp.bfloat16).astype(jnp.float32)
        return jnp.einsum('ngqk,knd->qngd', attn_probs, v_f32).astype(jnp.bfloat16)

    attn_out = lax.map(attend, (q_rot.reshape(blocks, QUERY_ROWS, KV_HEADS, GROUP_SIZE, HEAD_DIM), doc_id.reshape(blocks, QUERY_ROWS), tok_index.reshape(blocks, QUERY_ROWS)))
    mixed_out = jnp.dot(attn_out.reshape(TOKENS, Q_HEADS * HEAD_DIM), w_o, preferred_element_type=jnp.float32)
    y_out = (x_f32 + mixed_out).astype(jnp.bfloat16)
    return (y_out, k_rot, v_new)
```

```python
import jax
import jax.numpy as jnp
from jax import lax
from jax.experimental import pallas as pl
from jax.experimental.pallas import tpu as pltpu
from jax.sharding import PartitionSpec as P

MESH = pl.DeviceIdType.MESH
BF16, F32 = jnp.bfloat16, jnp.float32
LOG2E = 1.4426950408889634
KEY_BLOCK = 256


class Copies:
    def __init__(self, send_sem, recv_sem):
        self.send_sem, self.recv_sem, self.used = send_sem, recv_sem, 0

    def take(self, count):
        first = self.used
        self.used += count
        return first

    def make(self, index, src, dst, device):
        return pltpu.make_async_remote_copy(
            src_ref=src, dst_ref=dst, send_sem=self.send_sem.at[index], recv_sem=self.recv_sem.at[index],
            device_id=device, device_id_type=MESH)


class RingGather:
    def __init__(self, copies, right_dev, left_dev, here, left, right, far, at_right, at_left, at_far):
        first = copies.take(6)
        self.own = {}
        self.got = {}
        for half in (0, 1):
            self.own['r', half] = copies.make(first + half, here(half), at_right(half), right_dev)
            self.own['l', half] = copies.make(first + 2 + half, here(half), at_left(half), left_dev)
            self.got['r', half] = copies.make(first + half, left(half), left(half), right_dev)
            self.got['l', half] = copies.make(first + 2 + half, right(half), right(half), left_dev)
        self.passed = (copies.make(first + 4, left(0), at_far(0), right_dev),
                       copies.make(first + 5, right(1), at_far(1), left_dev))
        self.far_got = (copies.make(first + 4, far(0), far(0), right_dev),
                        copies.make(first + 5, far(1), far(1), left_dev))

    def send(self):
        for key in (('r', 0), ('l', 1), ('r', 1), ('l', 0)):
            self.own[key].start()

    def relay(self):
        self.got['r', 0].wait_recv()
        self.passed[0].start()
        self.got['l', 1].wait_recv()
        self.passed[1].start()

    def near(self):
        self.got['r', 1].wait_recv()
        self.got['l', 0].wait_recv()

    def last(self):
        self.far_got[0].wait_recv()
        self.far_got[1].wait_recv()

    def drain(self):
        for copy in self.own.values():
            copy.wait_send()
        for copy in self.passed:
            copy.wait_send()


class ChipGather:
    def __init__(self, copies, right_dev, left_dev, sib_dev, region, own, left, right, far, other):
        def at(owner):
            return lambda half: region(owner, half)
        self.ring = RingGather(copies, right_dev, left_dev, at(own), at(left), at(right), at(far),
                               at(own), at(own), lambda half: region(left if half == 0 else right, half))
        self.out, self.back = {}, {}
        for name, owner in (('own', own), ('left', left), ('right', right), ('far', far)):
            for half in (0, 1):
                index = copies.take(1)
                self.out[name, half] = copies.make(index, region(owner, half), region(owner, half), sib_dev)
                self.back[name, half] = copies.make(index, region(other(owner), half), region(other(owner), half), sib_dev)

    def send(self):
        self.ring.send()
        self.out['own', 0].start()
        self.out['own', 1].start()

    def relay(self):
        self.ring.relay()
        self.out['left', 0].start()
        self.out['right', 1].start()

    def near(self):
        self.ring.near()
        self.out['left', 1].start()
        self.out['right', 0].start()

    def last(self):
        self.ring.last()
        self.out['far', 0].start()
        self.out['far', 1].start()

    def finish(self):
        for copy in self.back.values():
            copy.wait_recv()

    def drain(self):
        self.ring.drain()
        for copy in self.out.values():
            copy.wait_send()


def layer_kernel(tp_size, cp_size, x_hbm, pos_hbm, gain_hbm, wq_hbm, wk_hbm, wv_hbm, wo_hbm, freq_hbm,
                 y_hbm, kc_hbm, vc_hbm,
                 xv, hv, gain_v, pos_v, freq_v, wkv, wq, wo, kv, qs, cos_v, sin_v, cap_v, scores, run_max, run_sum,
                 acc, oall, yall, load_sem, store_sem, send_sem, recv_sem):
    rows, width = xv.shape
    piece = rows // 2
    head_dim = wk_hbm.shape[1]
    half_dim = head_dim // 2
    head_cols = wq_hbm.shape[1]
    heads = head_cols // head_dim
    out_cols = width // tp_size
    low_rows = piece * cp_size
    share = head_cols // cp_size
    cut = (share // 2 + 15) // 16 * 16
    score_scale = head_dim ** -0.5 * LOG2E

    t = lax.axis_index('tp')
    c = lax.axis_index('cp')
    chips = cp_size // 2
    core = lax.rem(c, 2)
    chip = c // 2

    def tp_at(step):
        return lax.rem(t + step, tp_size)

    def cp_at(step):
        return lax.rem(chip + step, chips) * 2 + core

    def other(owner):
        return owner + 1 - 2 * core

    up, down = {'tp': tp_at(1)}, {'tp': tp_at(tp_size - 1)}
    right, left, sib = {'cp': cp_at(1)}, {'cp': cp_at(chips - 1)}, {'cp': other(c)}

    loads = {}

    def load(name, src, dst):
        loads[name] = pltpu.make_async_copy(src, dst, load_sem.at[len(loads)])
        loads[name].start()

    load('pos', pos_hbm, pos_v)
    load('freq', freq_hbm, freq_v)
    load('gain', gain_hbm, gain_v)
    for p in (0, 1):
        load(('x', p), x_hbm.at[pl.ds(p * piece, piece)], xv.at[pl.ds(p * piece, piece)])
    load('wk', wk_hbm, wkv.at[:, pl.ds(0, head_dim)])
    load('wv', wv_hbm, wkv.at[:, pl.ds(head_dim, head_dim)])
    q_chunks = ((0, 4), (4, heads - 4))
    for first, count in q_chunks:
        cols = pl.ds(first * head_dim, count * head_dim)
        load(('wq', first), wq_hbm.at[:, cols], wq.at[:, cols])
    own_cols = pl.multiple_of(t * out_cols, 128)
    load('wo', wo_hbm.at[:, pl.ds(own_cols, out_cols)], wo.at[0])

    barrier = pltpu.get_barrier_semaphore()
    peers = [{'tp': tp_at(step)} for step in range(1, tp_size)] + [right, left, sib]
    for peer in peers:
        pl.semaphore_signal(barrier, inc=1, device_id=peer, device_id_type=MESH)
    pl.semaphore_wait(barrier, len(peers))

    copies = Copies(send_sem, recv_sem)

    col_chunks = ((0, 512), (512, out_cols - 512))
    share_row = pl.multiple_of(c * share, 16)
    wo_out, wo_in = {}, {}
    for n, (start, size) in enumerate(col_chunks):
        for step in range(1, tp_size):
            index = copies.take(1)
            src_col = pl.multiple_of(tp_at(step) * out_cols + start, 128)
            wo_out[n, step] = copies.make(
                index, wo_hbm.at[pl.ds(share_row, share), pl.ds(src_col, size)],
                wo.at[tp_size - step, pl.ds(share_row, share), pl.ds(start, size)], {'tp': tp_at(step)})
            wo_out[n, step].start()
            landed = wo.at[tp_size - step, pl.ds(share_row, share), pl.ds(start, size)]
            wo_in[n, step] = copies.make(index, landed, landed, {'tp': tp_at(step)})

    def wo_region(n):
        start, size = col_chunks[n]

        def region(owner, half):
            first = pl.multiple_of(owner * share + (cut if half else 0), 16)
            return wo.at[pl.ds(1, tp_size - 1), pl.ds(first, share - cut if half else cut), pl.ds(start, size)]
        return region

    def kv_region(p):
        def region(owner, half):
            return kv.at[half, pl.ds(pl.multiple_of(p * low_rows + owner * piece, piece), piece)]
        return region

    def chip_gather(region):
        return ChipGather(copies, right, left, sib, region, c, cp_at(chips - 1), cp_at(1), cp_at(2), other)

    kv_gather = [chip_gather(kv_region(p)) for p in (0, 1)]
    wo_gather = [chip_gather(wo_region(n)) for n in range(len(col_chunks))]

    def tp_gather(buf, first, count, start, size):
        def at(slot):
            def region(half):
                return buf.at[slot, pl.ds(first + half * (count // 2), count // 2), pl.ds(start, size)]
            return region
        return RingGather(copies, up, down, at(0), at(3), at(1), at(2), at(3), at(1), at(2))

    o_gather = [tp_gather(oall, p * piece, piece, 0, head_cols) for p in (0, 1)]
    y_gather = {(p, n): tp_gather(yall, p * piece, piece, start, size)
                for p in (0, 1) for n, (start, size) in enumerate(col_chunks)}

    loads['pos'].wait()
    loads['freq'].wait()
    freq = jnp.concatenate([freq_v[...], freq_v[...]], axis=-1)
    lower = lax.broadcasted_iota(jnp.int32, (piece, head_dim), 1) < half_dim

    def pos_column(p):
        pos_row = pos_v[:, pl.ds(p * piece, piece)].astype(F32)
        return jnp.transpose(jnp.broadcast_to(pos_row, (piece, piece)))

    for p in (0, 1):
        angle = pos_column(p) * freq
        sine = jnp.sin(angle)
        cos_v[pl.ds(p * piece, piece), :] = jnp.cos(angle)
        sin_v[pl.ds(p * piece, piece), :] = jnp.where(lower, -sine, sine)

    def rope(vec, p):
        vec = vec.astype(F32)
        part = pl.ds(p * piece, piece)
        return (vec * cos_v[part, :] + pltpu.roll(vec, half_dim, 1) * sin_v[part, :]).astype(BF16)

    loads['gain'].wait()
    norm_rows = 16
    for p in (0, 1):
        loads['x', p].wait()

        def norm_step(step, _, p=p):
            part = pl.ds(pl.multiple_of(p * piece + step * norm_rows, norm_rows), norm_rows)
            x_f32 = xv[part, :].astype(F32)
            inv_rms = lax.rsqrt(jnp.mean(x_f32 * x_f32, axis=-1, keepdims=True) + 1e-5)
            hv[part, :] = (x_f32 * inv_rms * gain_v[...]).astype(BF16)
            return 0
        lax.fori_loop(0, piece // norm_rows, norm_step, 0)

    loads['wk'].wait()
    loads['wv'].wait()
    kv_new = jnp.dot(hv[...], wkv[...], preferred_element_type=F32).astype(BF16)
    for p in (0, 1):
        block = kv_new[p * piece:(p + 1) * piece]
        kv_region(p)(c, 0)[...] = rope(block[:, :head_dim], p)
        kv_region(p)(c, 1)[...] = block[:, head_dim:]
        kv_gather[p].send()
    stores = []

    def store(src, dst):
        stores.append(pltpu.make_async_copy(src, dst, store_sem.at[len(stores)]))
        stores[-1].start()

    for p in (0, 1):
        store(kv_region(p)(c, 0), kc_hbm.at[pl.ds(p * piece, piece)])
        store(kv_region(p)(c, 1), vc_hbm.at[pl.ds(p * piece, piece)])

    def queries(first, count):
        loads['wq', first].wait()
        new = jnp.dot(hv[...], wq[:, pl.ds(first * head_dim, count * head_dim)], preferred_element_type=F32).astype(BF16)
        for h in range(count):
            for p in (0, 1):
                qs[p, pl.ds((first + h) * piece, piece), :] = rope(
                    new[p * piece:(p + 1) * piece, h * head_dim:(h + 1) * head_dim], p)

    queries(*q_chunks[0])
    for p in (0, 1):
        kv_gather[p].relay()
    queries(*q_chunks[1])
    for p in (0, 1):
        kv_gather[p].near()
    for p in (0, 1):
        kv_gather[p].last()

    def attend(p):
        low_blocks = (chip + 1) if p == 0 else chips
        blocks = low_blocks if p == 0 else low_blocks + chips - chip
        piece_id = c if p == 0 else 2 * cp_size - 1 - c
        pos_col = pos_column(p)
        q_idx = (piece_id * piece).astype(F32) + lax.broadcasted_iota(jnp.int32, (piece, piece), 0).astype(F32)
        doc_start = q_idx - pos_col
        lane = lax.broadcasted_iota(jnp.int32, (piece, piece), 1).astype(F32)
        run_max[...] = jnp.full(run_max.shape, -jnp.inf, F32)
        run_sum[...] = jnp.zeros(run_sum.shape, F32)

        def key_rows(step):
            block = jnp.where(step < low_blocks, step, step - low_blocks + chip + chips)
            return block, pl.ds(pl.multiple_of(block * KEY_BLOCK, KEY_BLOCK), KEY_BLOCK)

        def score_step(step, _):
            block, part = key_rows(step)
            for half in (0, 1):
                owner = block * 2 + half
                owner_piece = jnp.where(owner < cp_size, owner, 3 * cp_size - 1 - owner)
                key_idx = (owner_piece * piece).astype(F32) + lane
                seen = (key_idx >= doc_start) & (key_idx <= q_idx)
                cap_v[:, half * piece:(half + 1) * piece] = jnp.where(seen, jnp.inf, -jnp.inf)
            raw = lax.dot_general(qs[p], kv[0, part, :], (((1,), (1,)), ((), ())), preferred_element_type=F32)
            for h in range(heads):
                mine = slice(h * piece, (h + 1) * piece)
                capped = jnp.minimum(raw[mine], cap_v[...])
                scores[step, mine, :] = capped
                run_max[mine, :] = jnp.maximum(run_max[mine, :], jnp.maximum(capped[:, :piece], capped[:, piece:]))
            return 0
        lax.fori_loop(0, blocks, score_step, 0)
        for h in range(heads):
            mine = slice(h * piece, (h + 1) * piece)
            top = jnp.max(run_max[mine, :], axis=-1, keepdims=True) * score_scale
            run_max[mine, :] = jnp.broadcast_to(top, (piece, piece))

        def sum_step(step, _):
            for h in range(heads):
                mine = slice(h * piece, (h + 1) * piece)
                shift = run_max[mine, :]
                run_sum[mine, :] += (jnp.exp2(scores[step, mine, :piece] * score_scale - shift)
                                     + jnp.exp2(scores[step, mine, piece:] * score_scale - shift))
            return 0
        lax.fori_loop(0, blocks, sum_step, 0)
        for h in range(heads):
            mine = slice(h * piece, (h + 1) * piece)
            total = jnp.sum(run_sum[mine, :], axis=-1, keepdims=True)
            run_max[mine, :] = run_max[mine, :] + jnp.broadcast_to(jnp.log2(total), (piece, piece))
        acc[...] = jnp.zeros(acc.shape, F32)

        def value_step(step, _):
            _, part = key_rows(step)
            shift = run_max[...]
            probs = jnp.concatenate([jnp.exp2(scores[step, :, :piece] * score_scale - shift).astype(BF16),
                                     jnp.exp2(scores[step, :, piece:] * score_scale - shift).astype(BF16)], axis=-1)
            acc[...] += jnp.dot(probs, kv[1, part, :], preferred_element_type=F32)
            return 0
        lax.fori_loop(0, blocks, value_step, 0)
        for h in range(heads):
            oall[0, pl.ds(p * piece, piece), h * head_dim:(h + 1) * head_dim] = (
                acc[h * piece:(h + 1) * piece, :].astype(BF16))

    for step in range(1, tp_size):
        wo_in[0, step].wait_recv()
    wo_gather[0].send()
    kv_gather[0].finish()
    kv_gather[1].finish()
    attend(0)
    o_gather[0].send()
    attend(1)
    o_gather[1].send()

    wo_gather[0].relay()
    o_gather[0].relay()
    for step in range(1, tp_size):
        wo_in[1, step].wait_recv()
    wo_gather[1].send()
    wo_gather[0].near()
    o_gather[0].near()
    o_gather[1].relay()
    wo_gather[0].last()
    o_gather[0].last()
    loads['wo'].wait()
    wo_gather[0].finish()

    def project(p, n):
        start, size = col_chunks[n]
        part = pl.ds(p * piece, piece)
        total = xv[part, pl.ds(pl.multiple_of(own_cols + start, 128), size)].astype(F32)
        mixed = jnp.dot(oall[0, part, :], wo[0, :, pl.ds(start, size)], preferred_element_type=F32)
        for slot in range(1, tp_size):
            mixed = mixed + jnp.dot(oall[slot, part, :], wo[slot, :, pl.ds(start, size)], preferred_element_type=F32)
        yall[0, part, pl.ds(start, size)] = (total + mixed).astype(BF16)
        y_gather[p, n].send()

    def put(p, n):
        start, size = col_chunks[n]
        part = pl.ds(p * piece, piece)
        for slot in range(tp_size):
            store(yall.at[slot, part, pl.ds(start, size)],
                  y_hbm.at[part, pl.ds(pl.multiple_of(tp_at(slot) * out_cols + start, 128), size)])

    project(0, 0)
    o_gather[1].near()
    wo_gather[1].relay()
    o_gather[1].last()
    project(1, 0)
    y_gather[0, 0].relay()
    wo_gather[1].near()
    wo_gather[1].last()
    wo_gather[1].finish()
    project(0, 1)
    y_gather[1, 0].relay()
    project(1, 1)
    y_gather[0, 0].near()
    y_gather[0, 0].last()
    put(0, 0)
    y_gather[0, 1].relay()
    y_gather[1, 0].near()
    y_gather[1, 0].last()
    put(1, 0)
    y_gather[1, 1].relay()
    y_gather[0, 1].near()
    y_gather[0, 1].last()
    put(0, 1)
    y_gather[1, 1].near()
    y_gather[1, 1].last()
    put(1, 1)

    for copy in wo_out.values():
        copy.wait_send()
    for gather in kv_gather + wo_gather + o_gather + list(y_gather.values()):
        gather.drain()
    for copy in stores:
        copy.wait()
    assert copies.used == send_sem.shape[0]


def solution(mesh):
    tp_size, cp_size = mesh.shape['tp'], mesh.shape['cp']

    def local_step(x_in, doc_id, pos_in_doc, norm_gain, w_q, w_k, w_v, w_o, inv_freq):
        del doc_id
        rows, width = x_in.shape
        piece = rows // 2
        head_dim = w_k.shape[1]
        head_cols = w_q.shape[1]
        heads = head_cols // head_dim
        out_cols = width // tp_size
        copies = 2 * (tp_size - 1) + 4 * 14 + 6 * 6
        stack = heads * piece
        y_out, k_new, v_new = pl.pallas_call(
            lambda *refs: layer_kernel(tp_size, cp_size, *refs),
            out_shape=(jax.ShapeDtypeStruct(x_in.shape, BF16), jax.ShapeDtypeStruct((rows, head_dim), BF16),
                       jax.ShapeDtypeStruct((rows, head_dim), BF16)),
            in_specs=[pl.BlockSpec(memory_space=pl.ANY)] * 8,
            out_specs=[pl.BlockSpec(memory_space=pl.ANY)] * 3,
            scratch_shapes=[
                pltpu.VMEM((rows, width), BF16),
                pltpu.VMEM((rows, width), BF16),
                pltpu.VMEM((1, width), F32),
                pltpu.VMEM((1, rows), jnp.int32),
                pltpu.VMEM((1, head_dim // 2), F32),
                pltpu.VMEM((width, 2 * head_dim), BF16),
                pltpu.VMEM((width, head_cols), BF16),
                pltpu.VMEM((tp_size, head_cols, out_cols), BF16),
                pltpu.VMEM((2, rows * cp_size, head_dim), BF16),
                pltpu.VMEM((2, stack, head_dim), BF16),
                pltpu.VMEM((rows, head_dim), F32),
                pltpu.VMEM((rows, head_dim), F32),
                pltpu.VMEM((piece, KEY_BLOCK), F32),
                pltpu.VMEM((rows * cp_size // KEY_BLOCK, stack, KEY_BLOCK), F32),
                pltpu.VMEM((stack, piece), F32),
                pltpu.VMEM((stack, piece), F32),
                pltpu.VMEM((stack, head_dim), F32),
                pltpu.VMEM((tp_size, rows, head_cols), BF16),
                pltpu.VMEM((tp_size, rows, out_cols), BF16),
                pltpu.SemaphoreType.DMA((10,)),
                pltpu.SemaphoreType.DMA((4 + 4 * tp_size,)),
                pltpu.SemaphoreType.DMA((copies,)),
                pltpu.SemaphoreType.DMA((copies,)),
            ],
            compiler_params=pltpu.CompilerParams(
                collective_id=0, has_side_effects=True, vmem_limit_bytes=60 * 1024 * 1024),
            name='layer',
        )(x_in, pos_in_doc.reshape(1, rows), norm_gain.reshape(1, width), w_q, w_k, w_v, w_o,
          inv_freq.reshape(1, head_dim // 2))
        kv_heads = 1
        return y_out, k_new.reshape(rows, kv_heads, head_dim), v_new.reshape(rows, kv_heads, head_dim)

    row_spec = P(('dp', 'cp'))
    in_specs = (P(('dp', 'cp'), None), row_spec, row_spec, P(), P(None, 'tp'), P(None, 'tp'), P(None, 'tp'), P('tp', None), P())
    out_specs = (P(('dp', 'cp'), None), P(('dp', 'cp'), 'tp', None), P(('dp', 'cp'), 'tp', None))
    return jax.shard_map(local_step, mesh=mesh, in_specs=in_specs, out_specs=out_specs, check_vma=False)
```

```python
import jax
import jax.numpy as jnp
from jax import lax
from jax.experimental import pallas as pl
from jax.experimental.pallas import tpu as pltpu
from jax.sharding import PartitionSpec as P

MESH = pl.DeviceIdType.MESH
BF16, F32 = jnp.bfloat16, jnp.float32
LOG2E = 1.4426950408889634
LOWEST = -1e38
KEY_BLOCK = 256


class Copies:
    def __init__(self, send_sem, recv_sem):
        self.send_sem, self.recv_sem, self.used = send_sem, recv_sem, 0

    def take(self, count):
        first = self.used
        self.used += count
        return first

    def make(self, index, src, dst, device):
        return pltpu.make_async_remote_copy(
            src_ref=src, dst_ref=dst, send_sem=self.send_sem.at[index], recv_sem=self.recv_sem.at[index],
            device_id=device, device_id_type=MESH)


class RingGather:
    def __init__(self, copies, right_dev, left_dev, here, left, right, far, at_right, at_left, at_far):
        first = copies.take(6)
        self.own = {}
        self.got = {}
        for half in (0, 1):
            self.own['r', half] = copies.make(first + half, here(half), at_right(half), right_dev)
            self.own['l', half] = copies.make(first + 2 + half, here(half), at_left(half), left_dev)
            self.got['r', half] = copies.make(first + half, left(half), left(half), right_dev)
            self.got['l', half] = copies.make(first + 2 + half, right(half), right(half), left_dev)
        self.passed = (copies.make(first + 4, left(0), at_far(0), right_dev),
                       copies.make(first + 5, right(1), at_far(1), left_dev))
        self.far_got = (copies.make(first + 4, far(0), far(0), right_dev),
                        copies.make(first + 5, far(1), far(1), left_dev))

    def send(self):
        for key in (('r', 0), ('l', 1), ('r', 1), ('l', 0)):
            self.own[key].start()

    def relay(self):
        self.got['r', 0].wait_recv()
        self.passed[0].start()
        self.got['l', 1].wait_recv()
        self.passed[1].start()

    def near(self):
        self.got['r', 1].wait_recv()
        self.got['l', 0].wait_recv()

    def last(self):
        self.far_got[0].wait_recv()
        self.far_got[1].wait_recv()

    def drain(self):
        for copy in self.own.values():
            copy.wait_send()
        for copy in self.passed:
            copy.wait_send()


class ChipGather:
    def __init__(self, copies, right_dev, left_dev, sib_dev, region, own, left, right, far, other):
        def at(owner):
            return lambda half: region(owner, half)
        self.ring = RingGather(copies, right_dev, left_dev, at(own), at(left), at(right), at(far),
                               at(own), at(own), lambda half: region(left if half == 0 else right, half))
        self.out, self.back = {}, {}
        for name, owner in (('own', own), ('left', left), ('right', right), ('far', far)):
            for half in (0, 1):
                index = copies.take(1)
                self.out[name, half] = copies.make(index, region(owner, half), region(owner, half), sib_dev)
                self.back[name, half] = copies.make(index, region(other(owner), half), region(other(owner), half), sib_dev)

    def send(self):
        self.ring.send()
        self.out['own', 0].start()
        self.out['own', 1].start()

    def relay(self):
        self.ring.relay()
        self.out['left', 0].start()
        self.out['right', 1].start()

    def near(self):
        self.ring.near()
        self.out['left', 1].start()
        self.out['right', 0].start()

    def last(self):
        self.ring.last()
        self.out['far', 0].start()
        self.out['far', 1].start()

    def finish(self):
        for copy in self.back.values():
            copy.wait_recv()

    def drain(self):
        self.ring.drain()
        for copy in self.out.values():
            copy.wait_send()


def layer_kernel(tp_size, cp_size, x_hbm, pos_hbm, gain_hbm, wq_hbm, wk_hbm, wv_hbm, wo_hbm, freq_hbm,
                 y_out, kc_out, vc_out,
                 xv, hv, gain_raw, gain_v, pos_v, freq_v, wkv, wq, wo, kv, qs, cos_v, sin_v, cap_v, scores, run_max,
                 run_sum, acc, oall, load_sem, send_sem, recv_sem):
    rows, width = xv.shape
    piece = rows // 2
    head_dim = wk_hbm.shape[1]
    half_dim = head_dim // 2
    head_cols = wq_hbm.shape[1]
    heads = head_cols // head_dim
    out_cols = width // tp_size
    low_rows = piece * cp_size
    share = head_cols // cp_size
    cut = (share // 2 + 15) // 16 * 16
    score_scale = head_dim ** -0.5 * LOG2E

    t = lax.axis_index('tp')
    c = lax.axis_index('cp')
    chips = cp_size // 2
    core = lax.rem(c, 2)
    chip = c // 2

    def tp_at(step):
        return lax.rem(t + step, tp_size)

    def cp_at(step):
        return lax.rem(chip + step, chips) * 2 + core

    def other(owner):
        return owner + 1 - 2 * core

    up, down = {'tp': tp_at(1)}, {'tp': tp_at(tp_size - 1)}
    right, left, sib = {'cp': cp_at(1)}, {'cp': cp_at(chips - 1)}, {'cp': other(c)}

    loads = {}

    def load(name, src, dst):
        loads[name] = pltpu.make_async_copy(src, dst, load_sem.at[len(loads)])
        loads[name].start()

    load('pos', pos_hbm, pos_v)
    load('freq', freq_hbm, freq_v)
    load('gain', gain_hbm, gain_raw)
    load(('x', 0), x_hbm.at[pl.ds(0, piece)], xv.at[pl.ds(0, piece)])
    load('wk', wk_hbm, wkv.at[:, pl.ds(0, head_dim)])
    load('wv', wv_hbm, wkv.at[:, pl.ds(head_dim, head_dim)])
    load(('x', 1), x_hbm.at[pl.ds(piece, piece)], xv.at[pl.ds(piece, piece)])
    own_cols = pl.multiple_of(t * out_cols, 128)
    q_chunks = ((0, 4), (4, heads - 4))

    barrier = pltpu.get_barrier_semaphore()
    peers = [{'tp': tp_at(step)} for step in range(1, tp_size)] + [right, left, sib]
    for peer in peers:
        pl.semaphore_signal(barrier, inc=1, device_id=peer, device_id_type=MESH)

    copies = Copies(send_sem, recv_sem)

    col_chunks = ((0, 512), (512, out_cols - 512))
    share_row = pl.multiple_of(c * share, 16)
    wo_out, wo_in = {}, {}
    for n, (start, size) in enumerate(col_chunks):
        for step in range(1, tp_size):
            index = copies.take(1)
            src_col = pl.multiple_of(tp_at(step) * out_cols + start, 128)
            wo_out[n, step] = copies.make(
                index, wo_hbm.at[pl.ds(share_row, share), pl.ds(src_col, size)],
                wo.at[tp_size - step, pl.ds(share_row, share), pl.ds(start, size)], {'tp': tp_at(step)})
            landed = wo.at[tp_size - step, pl.ds(share_row, share), pl.ds(start, size)]
            wo_in[n, step] = copies.make(index, landed, landed, {'tp': tp_at(step)})

    def wo_region(n):
        start, size = col_chunks[n]

        def region(owner, half):
            first = pl.multiple_of(owner * share + (cut if half else 0), 16)
            return wo.at[pl.ds(1, tp_size - 1), pl.ds(first, share - cut if half else cut), pl.ds(start, size)]
        return region

    def kv_region(p):
        def region(owner, half):
            return kv.at[half, pl.ds(pl.multiple_of(p * low_rows + owner * piece, piece), piece)]
        return region

    def chip_gather(region):
        return ChipGather(copies, right, left, sib, region, c, cp_at(chips - 1), cp_at(1), cp_at(2), other)

    kv_gather = [chip_gather(kv_region(p)) for p in (0, 1)]
    wo_gather = [chip_gather(wo_region(n)) for n in range(len(col_chunks))]

    def o_gather_of(p):
        def at(slot):
            return lambda half: oall.at[slot, pl.ds(p * piece + half * (piece // 2), piece // 2)]
        return RingGather(copies, up, down, at(0), at(3), at(1), at(2), at(3), at(1), at(2))

    def y_gather_of(p, n):
        start, size = col_chunks[n]

        def at(step):
            cols = pl.ds(pl.multiple_of(tp_at(step) * out_cols + start, 128), size)
            return lambda half: y_out.at[pl.ds(p * piece + half * (piece // 2), piece // 2), cols]

        def passed(half):
            return at(3 if half == 0 else 1)(half)
        return RingGather(copies, up, down, at(0), at(3), at(1), at(2), at(0), at(0), passed)

    o_gather = [o_gather_of(p) for p in (0, 1)]
    y_gather = {(p, n): y_gather_of(p, n) for p in (0, 1) for n in range(len(col_chunks))}

    loads['pos'].wait()
    loads['freq'].wait()
    freq = jnp.concatenate([freq_v[...], freq_v[...]], axis=-1)
    lower = lax.broadcasted_iota(jnp.int32, (piece, head_dim), 1) < half_dim

    def pos_column(p):
        pos_row = pos_v[:, pl.ds(p * piece, piece)].astype(F32)
        return jnp.transpose(jnp.broadcast_to(pos_row, (piece, piece)))

    angle = jnp.where(lower, pos_column(0), pos_column(1)) * freq
    cosine, sine = jnp.cos(angle), jnp.sin(angle)
    cosine_turned, sine_turned = pltpu.roll(cosine, half_dim, 1), pltpu.roll(sine, half_dim, 1)
    cos_v[0] = jnp.where(lower, cosine, cosine_turned)
    cos_v[1] = jnp.where(lower, cosine_turned, cosine)
    sin_v[0] = jnp.where(lower, -sine, sine_turned)
    sin_v[1] = jnp.where(lower, -sine_turned, sine)

    def rope(vec, p):
        vec = vec.astype(F32)
        return (vec * cos_v[p] + pltpu.roll(vec, half_dim, 1) * sin_v[p]).astype(BF16)

    loads['gain'].wait()
    for tile in range(width // 128):
        gain_v[:, tile * 128:(tile + 1) * 128] = gain_raw[tile:tile + 1, :]

    norm_rows = 32
    for p in (0, 1):
        loads['x', p].wait()

        def norm_step(step, _, p=p):
            part = pl.ds(pl.multiple_of(p * piece + step * norm_rows, norm_rows), norm_rows)
            x_f32 = xv[part, :].astype(F32)
            inv_rms = lax.rsqrt(jnp.mean(x_f32 * x_f32, axis=-1, keepdims=True) + 1e-5)
            hv[part, :] = (x_f32 * inv_rms * gain_v[...]).astype(BF16)
            return 0
        lax.fori_loop(0, piece // norm_rows, norm_step, 0)
        if p == 0:
            loads['wk'].wait()
            loads['wv'].wait()
            for first, count in q_chunks:
                cols = pl.ds(first * head_dim, count * head_dim)
                load(('wq', first), wq_hbm.at[:, cols], wq.at[:, cols])
            pl.semaphore_wait(barrier, len(peers))
        block = jnp.dot(hv[pl.ds(p * piece, piece), :], wkv[...], preferred_element_type=F32).astype(BF16)
        k_new, v_new = rope(block[:, :head_dim], p), block[:, head_dim:]
        kv_region(p)(c, 0)[...] = k_new
        kv_region(p)(c, 1)[...] = v_new
        kv_gather[p].send()
        kc_out[pl.ds(p * piece, piece), :] = k_new
        vc_out[pl.ds(p * piece, piece), :] = v_new
        if p == 0:
            for copy in wo_out.values():
                copy.start()
    load('wo', wo_hbm.at[:, pl.ds(own_cols, out_cols)], wo.at[0])

    def queries(first, count):
        loads['wq', first].wait()
        new = jnp.dot(hv[...], wq[:, pl.ds(first * head_dim, count * head_dim)], preferred_element_type=F32).astype(BF16)
        for h in range(count):
            for p in (0, 1):
                qs[p, pl.ds((first + h) * piece, piece), :] = rope(
                    new[p * piece:(p + 1) * piece, h * head_dim:(h + 1) * head_dim], p)

    def key_rows(block):
        return pl.ds(pl.multiple_of(block * KEY_BLOCK, KEY_BLOCK), KEY_BLOCK)

    def open_piece(p):
        run_max[...] = jnp.full(run_max.shape, LOWEST, F32)
        run_sum[...] = jnp.zeros(run_sum.shape, F32)
        acc[...] = jnp.zeros(acc.shape, F32)

    def score_blocks(p, count, block_of, slot_of):
        piece_id = c if p == 0 else 2 * cp_size - 1 - c
        q_idx = (piece_id * piece).astype(F32) + lax.broadcasted_iota(jnp.int32, (piece, piece), 0).astype(F32)
        doc_start = q_idx - pos_column(p)
        lane = lax.broadcasted_iota(jnp.int32, (piece, piece), 1).astype(F32)

        def score_step(step, _):
            block, slot = block_of(step), slot_of(step)
            for half in (0, 1):
                owner = block * 2 + half
                owner_piece = jnp.where(owner < cp_size, owner, 3 * cp_size - 1 - owner)
                key_idx = (owner_piece * piece).astype(F32) + lane
                seen = (key_idx >= doc_start) & (key_idx <= q_idx)
                cap_v[:, half * piece:(half + 1) * piece] = jnp.where(seen, jnp.inf, -jnp.inf)
            raw = lax.dot_general(qs[p], kv[0, key_rows(block), :], (((1,), (1,)), ((), ())),
                                  preferred_element_type=F32)
            for h in range(heads):
                mine = slice(h * piece, (h + 1) * piece)
                capped = jnp.minimum(raw[mine] * score_scale, cap_v[...])
                scores[slot, mine, :] = capped
                one, two = capped[:, :piece], capped[:, piece:]
                before = run_max[mine, :]
                top = jnp.maximum(before, jnp.maximum(one, two))
                run_max[mine, :] = top
                run_sum[mine, :] = (run_sum[mine, :] * jnp.exp2(before - top)
                                    + (jnp.exp2(one - top) + jnp.exp2(two - top)))
            return 0
        lax.fori_loop(0, count, score_step, 0)

    def close_scores():
        for h in range(heads):
            mine = slice(h * piece, (h + 1) * piece)
            lane_max = run_max[mine, :]
            top = jnp.broadcast_to(jnp.max(lane_max, axis=-1, keepdims=True), (piece, piece))
            total = jnp.sum(run_sum[mine, :] * jnp.exp2(lane_max - top), axis=-1, keepdims=True)
            run_max[mine, :] = top + jnp.broadcast_to(jnp.log2(total), (piece, piece))

    def value_blocks(count, block_of, slot_of):
        def value_step(step, _):
            block, slot = block_of(step), slot_of(step)
            shift = run_max[...]
            probs = jnp.concatenate([jnp.exp2(scores[slot, :, :piece] - shift).astype(BF16),
                                     jnp.exp2(scores[slot, :, piece:] - shift).astype(BF16)], axis=-1)
            acc[...] += jnp.dot(probs, kv[1, key_rows(block), :], preferred_element_type=F32)
            return 0
        lax.fori_loop(0, count, value_step, 0)

    def close_piece(p):
        for h in range(heads):
            oall[0, pl.ds(p * piece, piece), h * head_dim:(h + 1) * head_dim] = (
                acc[h * piece:(h + 1) * piece, :].astype(BF16))
        o_gather[p].send()

    def same(step):
        return step

    queries(*q_chunks[0])
    kv_gather[0].relay()
    queries(*q_chunks[1])
    kv_gather[1].relay()
    kv_gather[0].near()
    kv_gather[0].last()
    kv_gather[1].near()
    for step in range(1, tp_size):
        wo_in[0, step].wait_recv()
    wo_gather[0].send()
    kv_gather[0].finish()
    open_piece(0)
    score_blocks(0, chip + 1, same, same)
    close_scores()
    value_blocks(chip + 1, same, same)
    close_piece(0)
    kv_gather[1].last()
    open_piece(1)
    score_blocks(1, chips, same, same)
    kv_gather[1].finish()
    score_blocks(1, chips - chip, lambda step: step + chips + chip, lambda step: step + chips)
    close_scores()
    value_blocks(2 * chips - chip, lambda step: jnp.where(step < chips, step, step + chip), same)
    close_piece(1)

    wo_gather[0].relay()
    o_gather[0].relay()
    for step in range(1, tp_size):
        wo_in[1, step].wait_recv()
    wo_gather[1].send()
    wo_gather[0].near()
    o_gather[0].near()
    o_gather[1].relay()
    wo_gather[0].last()
    o_gather[0].last()
    loads['wo'].wait()
    wo_gather[0].finish()

    def project(p, n):
        start, size = col_chunks[n]
        part = pl.ds(p * piece, piece)
        total = xv[part, pl.ds(pl.multiple_of(own_cols + start, 128), size)].astype(F32)
        mixed = jnp.dot(oall[0, part, :], wo[0, :, pl.ds(start, size)], preferred_element_type=F32)
        for slot in range(1, tp_size):
            mixed = mixed + jnp.dot(oall[slot, part, :], wo[slot, :, pl.ds(start, size)], preferred_element_type=F32)
        y_out[part, pl.ds(pl.multiple_of(own_cols + start, 128), size)] = (total + mixed).astype(BF16)
        y_gather[p, n].send()

    project(0, 0)
    o_gather[1].near()
    wo_gather[1].relay()
    o_gather[1].last()
    project(1, 0)
    y_gather[0, 0].relay()
    wo_gather[1].near()
    wo_gather[1].last()
    wo_gather[1].finish()
    project(0, 1)
    y_gather[1, 0].relay()
    project(1, 1)
    y_gather[0, 0].near()
    y_gather[0, 0].last()
    y_gather[0, 1].relay()
    y_gather[1, 0].near()
    y_gather[1, 0].last()
    y_gather[1, 1].relay()
    y_gather[0, 1].near()
    y_gather[0, 1].last()
    y_gather[1, 1].near()
    y_gather[1, 1].last()

    for copy in wo_out.values():
        copy.wait_send()
    for gather in kv_gather + wo_gather + o_gather + list(y_gather.values()):
        gather.drain()
    assert copies.used == send_sem.shape[0]


def solution(mesh):
    tp_size, cp_size = mesh.shape['tp'], mesh.shape['cp']

    def local_step(x_in, doc_id, pos_in_doc, norm_gain, w_q, w_k, w_v, w_o, inv_freq):
        del doc_id
        rows, width = x_in.shape
        piece = rows // 2
        head_dim = w_k.shape[1]
        head_cols = w_q.shape[1]
        heads = head_cols // head_dim
        out_cols = width // tp_size
        copies = 2 * (tp_size - 1) + 4 * 14 + 6 * 6
        stack = heads * piece
        y_out, k_new, v_new = pl.pallas_call(
            lambda *refs: layer_kernel(tp_size, cp_size, *refs),
            out_shape=(jax.ShapeDtypeStruct(x_in.shape, BF16), jax.ShapeDtypeStruct((rows, head_dim), BF16),
                       jax.ShapeDtypeStruct((rows, head_dim), BF16)),
            in_specs=[pl.BlockSpec(memory_space=pltpu.HBM)] * 8,
            out_specs=[pl.BlockSpec(memory_space=pltpu.VMEM)] * 3,
            scratch_shapes=[
                pltpu.VMEM((rows, width), BF16),
                pltpu.VMEM((rows, width), BF16),
                pltpu.VMEM((width // 128, 128), F32),
                pltpu.VMEM((1, width), F32),
                pltpu.VMEM((1, rows), jnp.int32),
                pltpu.VMEM((1, head_dim // 2), F32),
                pltpu.VMEM((width, 2 * head_dim), BF16),
                pltpu.VMEM((width, head_cols), BF16),
                pltpu.VMEM((tp_size, head_cols, out_cols), BF16),
                pltpu.VMEM((2, rows * cp_size, head_dim), BF16),
                pltpu.VMEM((2, stack, head_dim), BF16),
                pltpu.VMEM((2, piece, head_dim), F32),
                pltpu.VMEM((2, piece, head_dim), F32),
                pltpu.VMEM((piece, KEY_BLOCK), F32),
                pltpu.VMEM((rows * cp_size // KEY_BLOCK, stack, KEY_BLOCK), F32),
                pltpu.VMEM((stack, piece), F32),
                pltpu.VMEM((stack, piece), F32),
                pltpu.VMEM((stack, head_dim), F32),
                pltpu.VMEM((tp_size, rows, head_cols), BF16),
                pltpu.SemaphoreType.DMA((10,)),
                pltpu.SemaphoreType.DMA((copies,)),
                pltpu.SemaphoreType.DMA((copies,)),
            ],
            compiler_params=pltpu.CompilerParams(
                collective_id=0, has_side_effects=True, vmem_limit_bytes=44 * 1024 * 1024),
            name='layer',
        )(*[pltpu.with_memory_space_constraint(a, pltpu.HBM) for a in (
            x_in, pos_in_doc.reshape(1, rows), norm_gain.reshape(width // 128, 128), w_q, w_k, w_v, w_o,
            inv_freq.reshape(1, head_dim // 2))])
        kv_heads = 1
        return y_out, k_new.reshape(rows, kv_heads, head_dim), v_new.reshape(rows, kv_heads, head_dim)

    row_spec = P(('dp', 'cp'))
    in_specs = (P(('dp', 'cp'), None), row_spec, row_spec, P(), P(None, 'tp'), P(None, 'tp'), P(None, 'tp'), P('tp', None), P())
    out_specs = (P(('dp', 'cp'), None), P(('dp', 'cp'), 'tp', None), P(('dp', 'cp'), 'tp', None))
    return jax.shard_map(local_step, mesh=mesh, in_specs=in_specs, out_specs=out_specs, check_vma=False)
```

```python
import jax
import jax.numpy as jnp
from jax import lax
from jax.experimental import pallas as pl
from jax.experimental.pallas import tpu as pltpu
from jax.sharding import PartitionSpec as P

MESH = pl.DeviceIdType.MESH
BF16, F32 = jnp.bfloat16, jnp.float32
LOG2E = 1.4426950408889634
LOWEST = -1e38
KEY_BLOCK = 256


class Copies:
    def __init__(self, send_sem, recv_sem):
        self.send_sem, self.recv_sem, self.used = send_sem, recv_sem, 0

    def take(self, count):
        first = self.used
        self.used += count
        return first

    def make(self, index, src, dst, device):
        return pltpu.make_async_remote_copy(
            src_ref=src, dst_ref=dst, send_sem=self.send_sem.at[index], recv_sem=self.recv_sem.at[index],
            device_id=device, device_id_type=MESH)


class RingGather:
    def __init__(self, copies, right_dev, left_dev, here, left, right, far, at_right, at_left, at_far):
        first = copies.take(6)
        self.own = {}
        self.got = {}
        for half in (0, 1):
            self.own['r', half] = copies.make(first + half, here(half), at_right(half), right_dev)
            self.own['l', half] = copies.make(first + 2 + half, here(half), at_left(half), left_dev)
            self.got['r', half] = copies.make(first + half, left(half), left(half), right_dev)
            self.got['l', half] = copies.make(first + 2 + half, right(half), right(half), left_dev)
        self.passed = (copies.make(first + 4, left(0), at_far(0), right_dev),
                       copies.make(first + 5, right(1), at_far(1), left_dev))
        self.far_got = (copies.make(first + 4, far(0), far(0), right_dev),
                        copies.make(first + 5, far(1), far(1), left_dev))

    def send(self):
        for key in (('r', 0), ('l', 1), ('r', 1), ('l', 0)):
            self.own[key].start()

    def relay(self):
        self.got['r', 0].wait_recv()
        self.passed[0].start()
        self.got['l', 1].wait_recv()
        self.passed[1].start()

    def near(self):
        self.got['r', 1].wait_recv()
        self.got['l', 0].wait_recv()

    def last(self):
        self.far_got[0].wait_recv()
        self.far_got[1].wait_recv()

    def drain(self):
        for copy in self.own.values():
            copy.wait_send()
        for copy in self.passed:
            copy.wait_send()


class ChipGather:
    def __init__(self, copies, right_dev, left_dev, sib_dev, region, own, left, right, far, other):
        def at(owner):
            return lambda half: region(owner, half)
        self.ring = RingGather(copies, right_dev, left_dev, at(own), at(left), at(right), at(far),
                               at(own), at(own), lambda half: region(left if half == 0 else right, half))
        self.out, self.back = {}, {}
        for name, owner in (('own', own), ('left', left), ('right', right), ('far', far)):
            for half in (0, 1):
                index = copies.take(1)
                self.out[name, half] = copies.make(index, region(owner, half), region(owner, half), sib_dev)
                self.back[name, half] = copies.make(index, region(other(owner), half), region(other(owner), half), sib_dev)

    def send(self):
        self.ring.send()
        self.out['own', 0].start()
        self.out['own', 1].start()

    def relay(self):
        self.ring.relay()
        self.out['left', 0].start()
        self.out['right', 1].start()

    def near(self):
        self.ring.near()
        self.out['left', 1].start()
        self.out['right', 0].start()

    def last(self):
        self.ring.last()
        self.out['far', 0].start()
        self.out['far', 1].start()

    def finish(self):
        for copy in self.back.values():
            copy.wait_recv()

    def drain(self):
        self.ring.drain()
        for copy in self.out.values():
            copy.wait_send()


class DirectGather:
    def __init__(self, copies, right_dev, left_dev, far_dev, sib_dev, region, own, left, right, far, other):
        self.out, self.got, self.hand, self.back = [], {}, {}, {}
        for name, dev, owner in (('left', right_dev, left), ('right', left_dev, right), ('far', far_dev, far)):
            index = copies.take(1)
            self.out.append(copies.make(index, region(own), region(own), dev))
            self.got[name] = copies.make(index, region(owner), region(owner), dev)
        for name, owner in (('own', own), ('left', left), ('right', right), ('far', far)):
            index = copies.take(1)
            self.hand[name] = copies.make(index, region(owner), region(owner), sib_dev)
            self.back[name] = copies.make(index, region(other(owner)), region(other(owner)), sib_dev)

    def send(self):
        for copy in self.out:
            copy.start()
        self.hand['own'].start()

    def near(self):
        for name in ('left', 'right'):
            self.got[name].wait_recv()
            self.hand[name].start()

    def last(self):
        self.got['far'].wait_recv()
        self.hand['far'].start()

    def finish(self):
        for name in ('left', 'right', 'far'):
            self.back[name].wait_recv()

    def drain(self):
        for copy in self.out + list(self.hand.values()):
            copy.wait_send()


def layer_kernel(tp_size, cp_size, x_hbm, pos_hbm, gain_hbm, wq_hbm, wk_hbm, wv_hbm, wo_hbm, freq_hbm,
                 y_out, kc_out, vc_out,
                 xv, hv, gain_raw, gain_v, pos_v, freq_v, wkv, wq, wo, kv, qs, cos_v, sin_v, cap_v, scores, run_max,
                 run_sum, acc, oall, load_sem, send_sem, recv_sem):
    rows, width = xv.shape
    piece = rows // 2
    head_dim = wk_hbm.shape[1]
    half_dim = head_dim // 2
    head_cols = wq_hbm.shape[1]
    heads = head_cols // head_dim
    out_cols = width // tp_size
    low_rows = piece * cp_size
    share = head_cols // cp_size
    cut = (share // 2 + 15) // 16 * 16
    score_scale = head_dim ** -0.5 * LOG2E

    t = lax.axis_index('tp')
    c = lax.axis_index('cp')
    chips = cp_size // 2
    core = lax.rem(c, 2)
    chip = c // 2

    def tp_at(step):
        return lax.rem(t + step, tp_size)

    def cp_at(step):
        return lax.rem(chip + step, chips) * 2 + core

    def other(owner):
        return owner + 1 - 2 * core

    up, down = {'tp': tp_at(1)}, {'tp': tp_at(tp_size - 1)}
    right, left, far, sib = {'cp': cp_at(1)}, {'cp': cp_at(chips - 1)}, {'cp': cp_at(2)}, {'cp': other(c)}

    loads = {}

    def load(name, src, dst):
        loads[name] = pltpu.make_async_copy(src, dst, load_sem.at[len(loads)])
        loads[name].start()

    load('pos', pos_hbm, pos_v)
    load('freq', freq_hbm, freq_v)
    load('gain', gain_hbm, gain_raw)
    load(('x', 0), x_hbm.at[pl.ds(0, piece)], xv.at[pl.ds(0, piece)])
    load('wk', wk_hbm, wkv.at[:, pl.ds(0, head_dim)])
    load('wv', wv_hbm, wkv.at[:, pl.ds(head_dim, head_dim)])
    load(('x', 1), x_hbm.at[pl.ds(piece, piece)], xv.at[pl.ds(piece, piece)])
    own_cols = pl.multiple_of(t * out_cols, 128)
    q_chunks = ((0, 4), (4, heads - 4))

    barrier = pltpu.get_barrier_semaphore()
    peers = [{'tp': tp_at(step)} for step in range(1, tp_size)] + [right, left, far, sib]
    for peer in peers:
        pl.semaphore_signal(barrier, inc=1, device_id=peer, device_id_type=MESH)

    copies = Copies(send_sem, recv_sem)

    col_chunks = ((0, 384), (384, 256), (640, out_cols - 640))
    share_row = pl.multiple_of(c * share, 16)
    wo_out, wo_in = {}, {}
    for n, (start, size) in enumerate(col_chunks):
        for step in range(1, tp_size):
            index = copies.take(1)
            src_col = pl.multiple_of(tp_at(step) * out_cols + start, 128)
            wo_out[n, step] = copies.make(
                index, wo_hbm.at[pl.ds(share_row, share), pl.ds(src_col, size)],
                wo.at[tp_size - step, pl.ds(share_row, share), pl.ds(start, size)], {'tp': tp_at(step)})
            landed = wo.at[tp_size - step, pl.ds(share_row, share), pl.ds(start, size)]
            wo_in[n, step] = copies.make(index, landed, landed, {'tp': tp_at(step)})

    def wo_region(n):
        start, size = col_chunks[n]

        def region(owner, half):
            first = pl.multiple_of(owner * share + (cut if half else 0), 16)
            return wo.at[pl.ds(1, tp_size - 1), pl.ds(first, share - cut if half else cut), pl.ds(start, size)]
        return region

    def kv_region(p, kind):
        def region(owner):
            return kv.at[kind, pl.ds(pl.multiple_of(p * low_rows + owner * piece, piece), piece)]
        return region

    def chip_gather(region):
        return ChipGather(copies, right, left, sib, region, c, cp_at(chips - 1), cp_at(1), cp_at(2), other)

    kv_gather = {(p, kind): DirectGather(copies, right, left, far, sib, kv_region(p, kind), c, cp_at(chips - 1), cp_at(1),
                                         cp_at(2), other) for p in (0, 1) for kind in (0, 1)}
    wo_gather = [chip_gather(wo_region(n)) for n in range(len(col_chunks))]

    def o_gather_of(p):
        def at(slot):
            return lambda half: oall.at[slot, pl.ds(p * piece + half * (piece // 2), piece // 2)]
        return RingGather(copies, up, down, at(0), at(3), at(1), at(2), at(3), at(1), at(2))

    def y_gather_of(p, n):
        start, size = col_chunks[n]

        def at(step):
            cols = pl.ds(pl.multiple_of(tp_at(step) * out_cols + start, 128), size)
            return lambda half: y_out.at[pl.ds(p * piece + half * (piece // 2), piece // 2), cols]

        def passed(half):
            return at(3 if half == 0 else 1)(half)
        return RingGather(copies, up, down, at(0), at(3), at(1), at(2), at(0), at(0), passed)

    o_gather = [o_gather_of(p) for p in (0, 1)]
    y_gather = {(p, n): y_gather_of(p, n) for p in (0, 1) for n in range(len(col_chunks))}

    loads['pos'].wait()
    loads['freq'].wait()
    freq = jnp.concatenate([freq_v[...], freq_v[...]], axis=-1)
    lower = lax.broadcasted_iota(jnp.int32, (piece, head_dim), 1) < half_dim

    def pos_column(p):
        pos_row = pos_v[:, pl.ds(p * piece, piece)].astype(F32)
        return jnp.transpose(jnp.broadcast_to(pos_row, (piece, piece)))

    angle = jnp.where(lower, pos_column(0), pos_column(1)) * freq
    cosine, sine = jnp.cos(angle), jnp.sin(angle)
    cosine_turned, sine_turned = pltpu.roll(cosine, half_dim, 1), pltpu.roll(sine, half_dim, 1)
    cos_v[0] = jnp.where(lower, cosine, cosine_turned)
    cos_v[1] = jnp.where(lower, cosine_turned, cosine)
    sin_v[0] = jnp.where(lower, -sine, sine_turned)
    sin_v[1] = jnp.where(lower, -sine_turned, sine)

    def rope(vec, p):
        vec = vec.astype(F32)
        return (vec * cos_v[p] + pltpu.roll(vec, half_dim, 1) * sin_v[p]).astype(BF16)

    loads['gain'].wait()
    for tile in range(width // 128):
        gain_v[:, tile * 128:(tile + 1) * 128] = gain_raw[tile:tile + 1, :]

    norm_rows = 32
    for p in (0, 1):
        loads['x', p].wait()

        def norm_step(step, _, p=p):
            part = pl.ds(pl.multiple_of(p * piece + step * norm_rows, norm_rows), norm_rows)
            x_f32 = xv[part, :].astype(F32)
            inv_rms = lax.rsqrt(jnp.mean(x_f32 * x_f32, axis=-1, keepdims=True) + 1e-5)
            hv[part, :] = (x_f32 * inv_rms * gain_v[...]).astype(BF16)
            return 0
        lax.fori_loop(0, piece // norm_rows, norm_step, 0)
        if p == 0:
            loads['wk'].wait()
            loads['wv'].wait()
            for first, count in q_chunks:
                cols = pl.ds(first * head_dim, count * head_dim)
                load(('wq', first), wq_hbm.at[:, cols], wq.at[:, cols])
            pl.semaphore_wait(barrier, len(peers))
            for copy in wo_out.values():
                copy.start()
        block = jnp.dot(hv[pl.ds(p * piece, piece), :], wkv[...], preferred_element_type=F32).astype(BF16)
        k_new, v_new = rope(block[:, :head_dim], p), block[:, head_dim:]
        kv_region(p, 0)(c)[...] = k_new
        kv_gather[p, 0].send()
        kv_region(p, 1)(c)[...] = v_new
        kv_gather[p, 1].send()
        kc_out[pl.ds(p * piece, piece), :] = k_new
        vc_out[pl.ds(p * piece, piece), :] = v_new
    load('wo', wo_hbm.at[:, pl.ds(own_cols, out_cols)], wo.at[0])

    def queries(first, count):
        loads['wq', first].wait()
        new = jnp.dot(hv[...], wq[:, pl.ds(first * head_dim, count * head_dim)], preferred_element_type=F32).astype(BF16)
        for h in range(count):
            for p in (0, 1):
                qs[p, pl.ds((first + h) * piece, piece), :] = rope(
                    new[p * piece:(p + 1) * piece, h * head_dim:(h + 1) * head_dim], p)

    def key_rows(block):
        return pl.ds(pl.multiple_of(block * KEY_BLOCK, KEY_BLOCK), KEY_BLOCK)

    run_max[...] = jnp.full(run_max.shape, LOWEST, F32)
    run_sum[...] = jnp.zeros(run_sum.shape, F32)

    def score(p, blocks):
        piece_id = c if p == 0 else 2 * cp_size - 1 - c
        q_idx = (piece_id * piece).astype(F32) + lax.broadcasted_iota(jnp.int32, (piece, piece), 0).astype(F32)
        doc_start = q_idx - pos_column(p)
        lane = lax.broadcasted_iota(jnp.int32, (piece, piece), 1).astype(F32)
        for n, block in enumerate(blocks):
            for half in (0, 1):
                owner = block * 2 + half
                owner_piece = jnp.where(owner < cp_size, owner, 3 * cp_size - 1 - owner)
                key_idx = (owner_piece * piece).astype(F32) + lane
                seen = (key_idx >= doc_start) & (key_idx <= q_idx)
                cap_v[n, :, half * piece:(half + 1) * piece] = jnp.where(seen, jnp.inf, -jnp.inf)
        raw = [lax.dot_general(qs[p], kv[0, key_rows(block), :], (((1,), (1,)), ((), ())), preferred_element_type=F32)
               for block in blocks]
        for h in range(heads):
            mine = slice(h * piece, (h + 1) * piece)
            parts = []
            for n, block in enumerate(blocks):
                capped = jnp.minimum(raw[n][mine] * score_scale, cap_v[n])
                scores[block + p * chips, mine, :] = capped
                parts += [capped[:, :piece], capped[:, piece:]]
            before = run_max[p, mine, :]
            top = before
            for part in parts:
                top = jnp.maximum(top, part)
            run_max[p, mine, :] = top
            total = run_sum[p, mine, :] * jnp.exp2(before - top)
            for part in parts:
                total = total + jnp.exp2(part - top)
            run_sum[p, mine, :] = total

    def score_loop(p, count, block_of):
        def step(i, _):
            score(p, [block_of(i)])
            return 0
        lax.fori_loop(0, count, step, 0)

    def close_scores(p):
        for h in range(heads):
            mine = slice(h * piece, (h + 1) * piece)
            lane_max = run_max[p, mine, :]
            top = jnp.broadcast_to(jnp.max(lane_max, axis=-1, keepdims=True), (piece, piece))
            total = jnp.sum(run_sum[p, mine, :] * jnp.exp2(lane_max - top), axis=-1, keepdims=True)
            run_max[p, mine, :] = top + jnp.broadcast_to(jnp.log2(total), (piece, piece))

    def value_loop(p, count, block_of):
        acc[...] = jnp.zeros(acc.shape, F32)

        def step(i, _):
            block = block_of(i)
            shift = run_max[p]
            probs = jnp.concatenate([jnp.exp2(scores[block + p * chips, :, :piece] - shift).astype(BF16),
                                     jnp.exp2(scores[block + p * chips, :, piece:] - shift).astype(BF16)], axis=-1)
            acc[...] += jnp.dot(probs, kv[1, key_rows(block), :], preferred_element_type=F32)
            return 0
        lax.fori_loop(0, count, step, 0)

    def close_piece(p):
        for h in range(heads):
            oall[0, pl.ds(p * piece, piece), h * head_dim:(h + 1) * head_dim] = (
                acc[h * piece:(h + 1) * piece, :].astype(BF16))
        o_gather[p].send()

    def project(p, n):
        start, size = col_chunks[n]
        part = pl.ds(p * piece, piece)
        total = xv[part, pl.ds(pl.multiple_of(own_cols + start, 128), size)].astype(F32)
        mixed = jnp.dot(oall[0, part, :], wo[0, :, pl.ds(start, size)], preferred_element_type=F32)
        for slot in range(1, tp_size):
            mixed = mixed + jnp.dot(oall[slot, part, :], wo[slot, :, pl.ds(start, size)], preferred_element_type=F32)
        y_out[part, pl.ds(pl.multiple_of(own_cols + start, 128), size)] = (total + mixed).astype(BF16)

    def wo_send(n):
        for step in range(1, tp_size):
            wo_in[n, step].wait_recv()
        wo_gather[n].send()

    queries(*q_chunks[0])
    kv_gather[0, 0].near()
    queries(*q_chunks[1])
    kv_gather[0, 0].back['own'].wait_recv()
    score(0, [chip])
    kv_gather[0, 0].last()
    kv_gather[0, 1].near()
    score(1, [chip])
    kv_gather[1, 0].back['own'].wait_recv()
    score(1, [chips + chip])
    wo_send(0)
    kv_gather[0, 0].finish()
    score_loop(0, chip, lambda i: i)
    close_scores(0)
    kv_gather[0, 1].last()
    kv_gather[0, 1].back['own'].wait_recv()
    kv_gather[0, 1].finish()
    value_loop(0, chip + 1, lambda i: i)
    close_piece(0)
    kv_gather[1, 0].near()
    kv_gather[1, 0].last()
    score(1, [lax.rem(chip + i, chips) for i in range(1, chips)])
    wo_gather[0].relay()
    wo_send(1)
    kv_gather[1, 1].near()
    kv_gather[1, 0].finish()
    score_loop(1, chips - 1 - chip, lambda i: chips + chip + 1 + i)
    kv_gather[1, 1].last()
    close_scores(1)
    o_gather[0].relay()
    kv_gather[1, 1].back['own'].wait_recv()
    kv_gather[1, 1].finish()
    value_loop(1, 2 * chips - chip, lambda i: jnp.where(i < chips, i, i + chip))
    close_piece(1)

    o_gather[0].near()
    wo_gather[0].near()
    wo_gather[0].last()
    o_gather[0].last()
    wo_gather[1].relay()
    wo_send(2)
    loads['wo'].wait()
    wo_gather[0].finish()
    project(0, 0)
    o_gather[1].relay()
    y_gather[0, 0].send()
    wo_gather[1].near()
    wo_gather[1].last()
    wo_gather[1].finish()
    project(0, 1)
    y_gather[0, 1].send()
    wo_gather[2].relay()
    o_gather[1].near()
    o_gather[1].last()
    project(1, 0)
    y_gather[1, 0].send()
    project(1, 1)
    y_gather[1, 1].send()
    y_gather[0, 0].relay()
    wo_gather[2].near()
    y_gather[0, 1].relay()
    wo_gather[2].last()
    wo_gather[2].finish()
    project(0, 2)
    y_gather[0, 2].send()
    project(1, 2)
    y_gather[1, 2].send()
    y_gather[1, 0].relay()
    y_gather[1, 1].relay()
    y_gather[0, 2].relay()
    y_gather[1, 2].relay()
    for gather in y_gather.values():
        gather.near()
        gather.last()

    for copy in wo_out.values():
        copy.wait_send()
    for gather in list(kv_gather.values()) + wo_gather + o_gather + list(y_gather.values()):
        gather.drain()
    assert copies.used == send_sem.shape[0]


def solution(mesh):
    tp_size, cp_size = mesh.shape['tp'], mesh.shape['cp']

    def local_step(x_in, doc_id, pos_in_doc, norm_gain, w_q, w_k, w_v, w_o, inv_freq):
        del doc_id
        rows, width = x_in.shape
        piece = rows // 2
        head_dim = w_k.shape[1]
        head_cols = w_q.shape[1]
        heads = head_cols // head_dim
        out_cols = width // tp_size
        copies = 3 * (tp_size - 1) + 4 * 7 + 3 * 14 + 8 * 6
        stack = heads * piece
        y_out, k_new, v_new = pl.pallas_call(
            lambda *refs: layer_kernel(tp_size, cp_size, *refs),
            out_shape=(jax.ShapeDtypeStruct(x_in.shape, BF16), jax.ShapeDtypeStruct((rows, head_dim), BF16),
                       jax.ShapeDtypeStruct((rows, head_dim), BF16)),
            in_specs=[pl.BlockSpec(memory_space=pltpu.HBM)] * 8,
            out_specs=[pl.BlockSpec(memory_space=pltpu.VMEM)] * 3,
            scratch_shapes=[
                pltpu.VMEM((rows, width), BF16),
                pltpu.VMEM((rows, width), BF16),
                pltpu.VMEM((width // 128, 128), F32),
                pltpu.VMEM((1, width), F32),
                pltpu.VMEM((1, rows), jnp.int32),
                pltpu.VMEM((1, head_dim // 2), F32),
                pltpu.VMEM((width, 2 * head_dim), BF16),
                pltpu.VMEM((width, head_cols), BF16),
                pltpu.VMEM((tp_size, head_cols, out_cols), BF16),
                pltpu.VMEM((2, rows * cp_size, head_dim), BF16),
                pltpu.VMEM((2, stack, head_dim), BF16),
                pltpu.VMEM((2, piece, head_dim), F32),
                pltpu.VMEM((2, piece, head_dim), F32),
                pltpu.VMEM((cp_size // 2 - 1, piece, KEY_BLOCK), F32),
                pltpu.VMEM((3 * cp_size // 2, stack, KEY_BLOCK), F32),
                pltpu.VMEM((2, stack, piece), F32),
                pltpu.VMEM((2, stack, piece), F32),
                pltpu.VMEM((stack, head_dim), F32),
                pltpu.VMEM((tp_size, rows, head_cols), BF16),
                pltpu.SemaphoreType.DMA((10,)),
                pltpu.SemaphoreType.DMA((copies,)),
                pltpu.SemaphoreType.DMA((copies,)),
            ],
            compiler_params=pltpu.CompilerParams(
                collective_id=0, has_side_effects=True, vmem_limit_bytes=44 * 1024 * 1024),
            name='layer',
        )(*[pltpu.with_memory_space_constraint(a, pltpu.HBM) for a in (
            x_in, pos_in_doc.reshape(1, rows), norm_gain.reshape(width // 128, 128), w_q, w_k, w_v, w_o,
            inv_freq.reshape(1, head_dim // 2))])
        kv_heads = 1
        return y_out, k_new.reshape(rows, kv_heads, head_dim), v_new.reshape(rows, kv_heads, head_dim)

    row_spec = P(('dp', 'cp'))
    in_specs = (P(('dp', 'cp'), None), row_spec, row_spec, P(), P(None, 'tp'), P(None, 'tp'), P(None, 'tp'), P('tp', None), P())
    out_specs = (P(('dp', 'cp'), None), P(('dp', 'cp'), 'tp', None), P(('dp', 'cp'), 'tp', None))
    return jax.shard_map(local_step, mesh=mesh, in_specs=in_specs, out_specs=out_specs, check_vma=False)
```

```python
import jax
import jax.numpy as jnp
from jax import lax
from jax.experimental import pallas as pl
from jax.experimental.pallas import tpu as pltpu
from jax.sharding import PartitionSpec as P

MESH = pl.DeviceIdType.MESH
BF16, F32 = jnp.bfloat16, jnp.float32
LOG2E = 1.4426950408889634
LOWEST = -1e38
KEY_BLOCK = 256


class Copies:
    def __init__(self, send_sem, recv_sem):
        self.send_sem, self.recv_sem, self.used = send_sem, recv_sem, 0

    def take(self, count):
        first = self.used
        self.used += count
        return first

    def make(self, index, src, dst, device):
        return pltpu.make_async_remote_copy(
            src_ref=src, dst_ref=dst, send_sem=self.send_sem.at[index], recv_sem=self.recv_sem.at[index],
            device_id=device, device_id_type=MESH)


class RingGather:
    def __init__(self, copies, right_dev, left_dev, here, left, right, far, at_right, at_left, at_far):
        first = copies.take(6)
        self.own = {}
        self.got = {}
        for half in (0, 1):
            self.own['r', half] = copies.make(first + half, here(half), at_right(half), right_dev)
            self.own['l', half] = copies.make(first + 2 + half, here(half), at_left(half), left_dev)
            self.got['r', half] = copies.make(first + half, left(half), left(half), right_dev)
            self.got['l', half] = copies.make(first + 2 + half, right(half), right(half), left_dev)
        self.passed = (copies.make(first + 4, left(0), at_far(0), right_dev),
                       copies.make(first + 5, right(1), at_far(1), left_dev))
        self.far_got = (copies.make(first + 4, far(0), far(0), right_dev),
                        copies.make(first + 5, far(1), far(1), left_dev))

    def send(self):
        for key in (('r', 0), ('l', 1), ('r', 1), ('l', 0)):
            self.own[key].start()

    def relay(self):
        self.got['r', 0].wait_recv()
        self.passed[0].start()
        self.got['l', 1].wait_recv()
        self.passed[1].start()

    def near(self):
        self.got['r', 1].wait_recv()
        self.got['l', 0].wait_recv()

    def last(self):
        self.far_got[0].wait_recv()
        self.far_got[1].wait_recv()

    def drain(self):
        for copy in self.own.values():
            copy.wait_send()
        for copy in self.passed:
            copy.wait_send()


class ChipGather:
    def __init__(self, copies, right_dev, left_dev, sib_dev, region, own, left, right, far, other):
        def at(owner):
            return lambda half: region(owner, half)
        self.ring = RingGather(copies, right_dev, left_dev, at(own), at(left), at(right), at(far),
                               at(own), at(own), lambda half: region(left if half == 0 else right, half))
        self.out, self.back = {}, {}
        for name, owner in (('own', own), ('left', left), ('right', right), ('far', far)):
            for half in (0, 1):
                index = copies.take(1)
                self.out[name, half] = copies.make(index, region(owner, half), region(owner, half), sib_dev)
                self.back[name, half] = copies.make(index, region(other(owner), half), region(other(owner), half), sib_dev)

    def send(self):
        self.ring.send()
        self.out['own', 0].start()
        self.out['own', 1].start()

    def relay(self):
        self.ring.relay()
        self.out['left', 0].start()
        self.out['right', 1].start()

    def near(self):
        self.ring.near()
        self.out['left', 1].start()
        self.out['right', 0].start()

    def last(self):
        self.ring.last()
        self.out['far', 0].start()
        self.out['far', 1].start()

    def finish(self):
        for copy in self.back.values():
            copy.wait_recv()

    def drain(self):
        self.ring.drain()
        for copy in self.out.values():
            copy.wait_send()


class DirectGather:
    def __init__(self, copies, right_dev, left_dev, far_dev, sib_dev, region, own, left, right, far, other):
        self.out, self.got, self.hand, self.back = [], {}, {}, {}
        for name, dev, owner in (('left', right_dev, left), ('right', left_dev, right), ('far', far_dev, far)):
            index = copies.take(1)
            self.out.append(copies.make(index, region(own), region(own), dev))
            self.got[name] = copies.make(index, region(owner), region(owner), dev)
        for name, owner in (('own', own), ('left', left), ('right', right), ('far', far)):
            index = copies.take(1)
            self.hand[name] = copies.make(index, region(owner), region(owner), sib_dev)
            self.back[name] = copies.make(index, region(other(owner)), region(other(owner)), sib_dev)

    def send(self):
        for copy in self.out:
            copy.start()
        self.hand['own'].start()

    def near(self):
        for name in ('left', 'right'):
            self.got[name].wait_recv()
            self.hand[name].start()

    def last(self):
        self.got['far'].wait_recv()
        self.hand['far'].start()

    def finish(self):
        for name in ('left', 'right', 'far'):
            self.back[name].wait_recv()

    def drain(self):
        for copy in self.out + list(self.hand.values()):
            copy.wait_send()


def layer_kernel(tp_size, cp_size, x_hbm, pos_hbm, gain_hbm, wq_hbm, wk_hbm, wv_hbm, wo_hbm, freq_hbm,
                 y_out, kv_out,
                 xv, hv, gain_raw, gain_v, pos_v, freq_v, wkv, wq, wo, kv, qs, cos_v, sin_v, cap_v, scores, run_max,
                 run_sum, acc, oall, load_sem, send_sem, recv_sem):
    rows, width = xv.shape
    piece = rows // 2
    head_dim = wk_hbm.shape[1]
    half_dim = head_dim // 2
    head_cols = wq_hbm.shape[1]
    heads = head_cols // head_dim
    out_cols = width // tp_size
    low_rows = piece * cp_size
    share = head_cols // cp_size
    cut = (share // 2 + 15) // 16 * 16
    score_scale = head_dim ** -0.5 * LOG2E

    t = lax.axis_index('tp')
    c = lax.axis_index('cp')
    chips = cp_size // 2
    core = lax.rem(c, 2)
    chip = c // 2

    def tp_at(step):
        return lax.rem(t + step, tp_size)

    def cp_at(step):
        return lax.rem(chip + step, chips) * 2 + core

    def other(owner):
        return owner + 1 - 2 * core

    up, down = {'tp': tp_at(1)}, {'tp': tp_at(tp_size - 1)}
    right, left, far, sib = {'cp': cp_at(1)}, {'cp': cp_at(chips - 1)}, {'cp': cp_at(2)}, {'cp': other(c)}

    loads = {}

    def load(name, src, dst):
        loads[name] = pltpu.make_async_copy(src, dst, load_sem.at[len(loads)])
        loads[name].start()

    load('pos', pos_hbm, pos_v)
    load('freq', freq_hbm, freq_v)
    load('gain', gain_hbm, gain_raw)
    load(('x', 0), x_hbm.at[pl.ds(0, piece)], xv.at[pl.ds(0, piece)])
    load('wk', wk_hbm, wkv.at[:, pl.ds(0, head_dim)])
    load('wv', wv_hbm, wkv.at[:, pl.ds(head_dim, head_dim)])
    load(('x', 1), x_hbm.at[pl.ds(piece, piece)], xv.at[pl.ds(piece, piece)])
    own_cols = pl.multiple_of(t * out_cols, 128)
    q_chunks = ((0, 4), (4, heads - 4))

    barrier = pltpu.get_barrier_semaphore()
    peers = [{'tp': tp_at(step)} for step in range(1, tp_size)] + [right, left, far, sib]
    for peer in peers:
        pl.semaphore_signal(barrier, inc=1, device_id=peer, device_id_type=MESH)

    copies = Copies(send_sem, recv_sem)

    col_chunks = ((0, 384), (384, 256), (640, out_cols - 640))
    share_row = pl.multiple_of(c * share, 16)
    wo_out, wo_in = {}, {}
    for n, (start, size) in enumerate(col_chunks):
        for step in range(1, tp_size):
            index = copies.take(1)
            src_col = pl.multiple_of(tp_at(step) * out_cols + start, 128)
            wo_out[n, step] = copies.make(
                index, wo_hbm.at[pl.ds(share_row, share), pl.ds(src_col, size)],
                wo.at[tp_size - step, pl.ds(share_row, share), pl.ds(start, size)], {'tp': tp_at(step)})
            landed = wo.at[tp_size - step, pl.ds(share_row, share), pl.ds(start, size)]
            wo_in[n, step] = copies.make(index, landed, landed, {'tp': tp_at(step)})

    def wo_region(n):
        start, size = col_chunks[n]

        def region(owner, half):
            first = pl.multiple_of(owner * share + (cut if half else 0), 16)
            return wo.at[pl.ds(1, tp_size - 1), pl.ds(first, share - cut if half else cut), pl.ds(start, size)]
        return region

    def kv_region(p, kind):
        def region(owner):
            return kv.at[kind, pl.ds(pl.multiple_of(p * low_rows + owner * piece, piece), piece)]
        return region

    def chip_gather(region):
        return ChipGather(copies, right, left, sib, region, c, cp_at(chips - 1), cp_at(1), cp_at(2), other)

    kv_gather = {(p, kind): DirectGather(copies, right, left, far, sib, kv_region(p, kind), c, cp_at(chips - 1), cp_at(1),
                                         cp_at(2), other) for p in (0, 1) for kind in (0, 1)}
    wo_gather = [chip_gather(wo_region(n)) for n in range(len(col_chunks))]

    def o_gather_of(p):
        def at(slot):
            return lambda half: oall.at[slot, pl.ds(p * piece + half * (piece // 2), piece // 2)]
        return RingGather(copies, up, down, at(0), at(3), at(1), at(2), at(3), at(1), at(2))

    def y_gather_of(p, n):
        start, size = col_chunks[n]

        def at(step):
            cols = pl.ds(pl.multiple_of(tp_at(step) * out_cols + start, 128), size)
            return lambda half: y_out.at[pl.ds(p * piece + half * (piece // 2), piece // 2), cols]

        def passed(half):
            return at(3 if half == 0 else 1)(half)
        return RingGather(copies, up, down, at(0), at(3), at(1), at(2), at(0), at(0), passed)

    o_gather = [o_gather_of(p) for p in (0, 1)]
    y_gather = {(p, n): y_gather_of(p, n) for p in (0, 1) for n in range(len(col_chunks))}

    loads['pos'].wait()
    loads['freq'].wait()
    freq = jnp.concatenate([freq_v[...], freq_v[...]], axis=-1)
    lower = lax.broadcasted_iota(jnp.int32, (piece, head_dim), 1) < half_dim

    def pos_column(p):
        pos_row = pos_v[:, pl.ds(p * piece, piece)].astype(F32)
        return jnp.transpose(jnp.broadcast_to(pos_row, (piece, piece)))

    angle = jnp.where(lower, pos_column(0), pos_column(1)) * freq
    cosine, sine = jnp.cos(angle), jnp.sin(angle)
    cosine_turned, sine_turned = pltpu.roll(cosine, half_dim, 1), pltpu.roll(sine, half_dim, 1)
    cos_v[0] = jnp.where(lower, cosine, cosine_turned)
    cos_v[1] = jnp.where(lower, cosine_turned, cosine)
    sin_v[0] = jnp.where(lower, -sine, sine_turned)
    sin_v[1] = jnp.where(lower, -sine_turned, sine)

    def rope(vec, p):
        vec = vec.astype(F32)
        return (vec * cos_v[p] + pltpu.roll(vec, half_dim, 1) * sin_v[p]).astype(BF16)

    loads['gain'].wait()
    for tile in range(width // 128):
        gain_v[:, tile * 128:(tile + 1) * 128] = gain_raw[tile:tile + 1, :]

    norm_rows = 32
    for p in (0, 1):
        loads['x', p].wait()

        def norm_step(step, _, p=p):
            part = pl.ds(pl.multiple_of(p * piece + step * norm_rows, norm_rows), norm_rows)
            x_f32 = xv[part, :].astype(F32)
            inv_rms = lax.rsqrt(jnp.mean(x_f32 * x_f32, axis=-1, keepdims=True) + 1e-5)
            hv[part, :] = (x_f32 * inv_rms * gain_v[...]).astype(BF16)
            return 0
        lax.fori_loop(0, piece // norm_rows, norm_step, 0)
        if p == 0:
            loads['wk'].wait()
            loads['wv'].wait()
            for first, count in q_chunks:
                cols = pl.ds(first * head_dim, count * head_dim)
                load(('wq', first), wq_hbm.at[:, cols], wq.at[:, cols])
            pl.semaphore_wait(barrier, len(peers))
            for copy in wo_out.values():
                copy.start()
        block = jnp.dot(hv[pl.ds(p * piece, piece), :], wkv[...], preferred_element_type=F32).astype(BF16)
        k_new, v_new = rope(block[:, :head_dim], p), block[:, head_dim:]
        kv_region(p, 0)(c)[...] = k_new
        kv_gather[p, 0].send()
        kv_region(p, 1)(c)[...] = v_new
        kv_gather[p, 1].send()
        kv_out[0, pl.ds(p * piece, piece), :] = k_new
        kv_out[1, pl.ds(p * piece, piece), :] = v_new
    load('wo', wo_hbm.at[:, pl.ds(own_cols, out_cols)], wo.at[0])

    def queries(first, count):
        loads['wq', first].wait()
        new = jnp.dot(hv[...], wq[:, pl.ds(first * head_dim, count * head_dim)], preferred_element_type=F32).astype(BF16)
        for h in range(count):
            for p in (0, 1):
                qs[p, pl.ds((first + h) * piece, piece), :] = rope(
                    new[p * piece:(p + 1) * piece, h * head_dim:(h + 1) * head_dim], p)

    def key_rows(block):
        return pl.ds(pl.multiple_of(block * KEY_BLOCK, KEY_BLOCK), KEY_BLOCK)

    run_max[...] = jnp.full(run_max.shape, LOWEST, F32)
    run_sum[...] = jnp.zeros(run_sum.shape, F32)

    def score(p, blocks):
        piece_id = c if p == 0 else 2 * cp_size - 1 - c
        q_idx = (piece_id * piece).astype(F32) + lax.broadcasted_iota(jnp.int32, (piece, piece), 0).astype(F32)
        doc_start = q_idx - pos_column(p)
        lane = lax.broadcasted_iota(jnp.int32, (piece, piece), 1).astype(F32)
        for n, block in enumerate(blocks):
            for half in (0, 1):
                owner = block * 2 + half
                owner_piece = jnp.where(owner < cp_size, owner, 3 * cp_size - 1 - owner)
                key_idx = (owner_piece * piece).astype(F32) + lane
                seen = (key_idx >= doc_start) & (key_idx <= q_idx)
                cap_v[n, :, half * piece:(half + 1) * piece] = jnp.where(seen, jnp.inf, -jnp.inf)
        raw = [lax.dot_general(qs[p], kv[0, key_rows(block), :], (((1,), (1,)), ((), ())), preferred_element_type=F32)
               for block in blocks]
        for h in range(heads):
            mine = slice(h * piece, (h + 1) * piece)
            parts = []
            for n, block in enumerate(blocks):
                capped = jnp.minimum(raw[n][mine] * score_scale, cap_v[n])
                scores[block + p * chips, mine, :] = capped
                parts += [capped[:, :piece], capped[:, piece:]]
            before = run_max[p, mine, :]
            top = before
            for part in parts:
                top = jnp.maximum(top, part)
            run_max[p, mine, :] = top
            total = run_sum[p, mine, :] * jnp.exp2(before - top)
            for part in parts:
                total = total + jnp.exp2(part - top)
            run_sum[p, mine, :] = total

    def score_loop(p, count, block_of):
        def step(i, _):
            score(p, [block_of(i)])
            return 0
        lax.fori_loop(0, count, step, 0)

    def close_scores(p):
        for h in range(heads):
            mine = slice(h * piece, (h + 1) * piece)
            lane_max = run_max[p, mine, :]
            top = jnp.broadcast_to(jnp.max(lane_max, axis=-1, keepdims=True), (piece, piece))
            total = jnp.sum(run_sum[p, mine, :] * jnp.exp2(lane_max - top), axis=-1, keepdims=True)
            run_max[p, mine, :] = top + jnp.broadcast_to(jnp.log2(total), (piece, piece))

    def value_loop(p, count, block_of):
        acc[...] = jnp.zeros(acc.shape, F32)

        def step(i, _):
            block = block_of(i)
            shift = run_max[p]
            probs = jnp.concatenate([jnp.exp2(scores[block + p * chips, :, :piece] - shift).astype(BF16),
                                     jnp.exp2(scores[block + p * chips, :, piece:] - shift).astype(BF16)], axis=-1)
            acc[...] += jnp.dot(probs, kv[1, key_rows(block), :], preferred_element_type=F32)
            return 0
        lax.fori_loop(0, count, step, 0)

    def close_piece(p):
        for h in range(heads):
            oall[0, pl.ds(p * piece, piece), h * head_dim:(h + 1) * head_dim] = (
                acc[h * piece:(h + 1) * piece, :].astype(BF16))
        o_gather[p].send()

    def project(p, n):
        start, size = col_chunks[n]
        part = pl.ds(p * piece, piece)
        total = xv[part, pl.ds(pl.multiple_of(own_cols + start, 128), size)].astype(F32)
        mixed = jnp.dot(oall[0, part, :], wo[0, :, pl.ds(start, size)], preferred_element_type=F32)
        for slot in range(1, tp_size):
            mixed = mixed + jnp.dot(oall[slot, part, :], wo[slot, :, pl.ds(start, size)], preferred_element_type=F32)
        y_out[part, pl.ds(pl.multiple_of(own_cols + start, 128), size)] = (total + mixed).astype(BF16)

    def wo_send(n):
        for step in range(1, tp_size):
            wo_in[n, step].wait_recv()
        wo_gather[n].send()

    queries(*q_chunks[0])
    kv_gather[0, 0].near()
    queries(*q_chunks[1])
    kv_gather[0, 0].back['own'].wait_recv()
    score(0, [chip])
    kv_gather[0, 0].last()
    kv_gather[0, 1].near()
    score(1, [chip])
    kv_gather[1, 0].back['own'].wait_recv()
    score(1, [chips + chip])
    wo_send(0)
    kv_gather[0, 0].finish()
    score_loop(0, chip, lambda i: i)
    close_scores(0)
    kv_gather[0, 1].last()
    kv_gather[0, 1].back['own'].wait_recv()
    kv_gather[0, 1].finish()
    value_loop(0, chip + 1, lambda i: i)
    close_piece(0)
    kv_gather[1, 0].near()
    kv_gather[1, 0].last()
    score(1, [lax.rem(chip + i, chips) for i in range(1, chips)])
    wo_gather[0].relay()
    wo_send(1)
    kv_gather[1, 1].near()
    kv_gather[1, 0].finish()
    score_loop(1, chips - 1 - chip, lambda i: chips + chip + 1 + i)
    kv_gather[1, 1].last()
    close_scores(1)
    o_gather[0].relay()
    kv_gather[1, 1].back['own'].wait_recv()
    kv_gather[1, 1].finish()
    value_loop(1, 2 * chips - chip, lambda i: jnp.where(i < chips, i, i + chip))
    close_piece(1)

    o_gather[0].near()
    wo_gather[0].near()
    wo_gather[0].last()
    o_gather[0].last()
    wo_gather[1].relay()
    wo_send(2)
    loads['wo'].wait()
    wo_gather[0].finish()
    project(0, 0)
    o_gather[1].relay()
    y_gather[0, 0].send()
    wo_gather[1].near()
    wo_gather[1].last()
    wo_gather[1].finish()
    project(0, 1)
    y_gather[0, 1].send()
    wo_gather[2].relay()
    o_gather[1].near()
    o_gather[1].last()
    project(1, 0)
    y_gather[1, 0].send()
    project(1, 1)
    y_gather[1, 1].send()
    y_gather[0, 0].relay()
    wo_gather[2].near()
    y_gather[0, 1].relay()
    wo_gather[2].last()
    wo_gather[2].finish()
    project(0, 2)
    y_gather[0, 2].send()
    project(1, 2)
    y_gather[1, 2].send()
    y_gather[1, 0].relay()
    y_gather[1, 1].relay()
    y_gather[0, 2].relay()
    y_gather[1, 2].relay()
    for gather in y_gather.values():
        gather.near()
        gather.last()

    for copy in wo_out.values():
        copy.wait_send()
    for gather in list(kv_gather.values()) + wo_gather + o_gather + list(y_gather.values()):
        gather.drain()
    assert copies.used == send_sem.shape[0]


def solution(mesh):
    tp_size, cp_size = mesh.shape['tp'], mesh.shape['cp']

    def local_step(x_in, doc_id, pos_in_doc, norm_gain, w_q, w_k, w_v, w_o, inv_freq):
        del doc_id
        rows, width = x_in.shape
        piece = rows // 2
        head_dim = w_k.shape[1]
        head_cols = w_q.shape[1]
        heads = head_cols // head_dim
        out_cols = width // tp_size
        copies = 3 * (tp_size - 1) + 4 * 7 + 3 * 14 + 8 * 6
        stack = heads * piece
        y_out, kv_new = pl.pallas_call(
            lambda *refs: layer_kernel(tp_size, cp_size, *refs),
            out_shape=(jax.ShapeDtypeStruct(x_in.shape, BF16), jax.ShapeDtypeStruct((2, rows, head_dim), BF16)),
            in_specs=[pl.BlockSpec(memory_space=pltpu.HBM)] * 8,
            out_specs=[pl.BlockSpec(memory_space=pltpu.VMEM)] * 2,
            scratch_shapes=[
                pltpu.VMEM((rows, width), BF16),
                pltpu.VMEM((rows, width), BF16),
                pltpu.VMEM((width // 128, 128), F32),
                pltpu.VMEM((1, width), F32),
                pltpu.VMEM((1, rows), jnp.int32),
                pltpu.VMEM((1, head_dim // 2), F32),
                pltpu.VMEM((width, 2 * head_dim), BF16),
                pltpu.VMEM((width, head_cols), BF16),
                pltpu.VMEM((tp_size, head_cols, out_cols), BF16),
                pltpu.VMEM((2, rows * cp_size, head_dim), BF16),
                pltpu.VMEM((2, stack, head_dim), BF16),
                pltpu.VMEM((2, piece, head_dim), F32),
                pltpu.VMEM((2, piece, head_dim), F32),
                pltpu.VMEM((cp_size // 2 - 1, piece, KEY_BLOCK), F32),
                pltpu.VMEM((3 * cp_size // 2, stack, KEY_BLOCK), F32),
                pltpu.VMEM((2, stack, piece), F32),
                pltpu.VMEM((2, stack, piece), F32),
                pltpu.VMEM((stack, head_dim), F32),
                pltpu.VMEM((tp_size, rows, head_cols), BF16),
                pltpu.SemaphoreType.DMA((10,)),
                pltpu.SemaphoreType.DMA((copies,)),
                pltpu.SemaphoreType.DMA((copies,)),
            ],
            compiler_params=pltpu.CompilerParams(
                collective_id=0, has_side_effects=True, vmem_limit_bytes=44 * 1024 * 1024),
            name='layer',
        )(*[pltpu.with_memory_space_constraint(a, pltpu.HBM) for a in (
            x_in, pos_in_doc.reshape(1, rows), norm_gain.reshape(width // 128, 128), w_q, w_k, w_v, w_o,
            inv_freq.reshape(1, head_dim // 2))])
        kv_heads = 1
        return y_out, kv_new[0].reshape(rows, kv_heads, head_dim), kv_new[1].reshape(rows, kv_heads, head_dim)

    row_spec = P(('dp', 'cp'))
    in_specs = (P(('dp', 'cp'), None), row_spec, row_spec, P(), P(None, 'tp'), P(None, 'tp'), P(None, 'tp'), P('tp', None), P())
    out_specs = (P(('dp', 'cp'), None), P(('dp', 'cp'), 'tp', None), P(('dp', 'cp'), 'tp', None))
    return jax.shard_map(local_step, mesh=mesh, in_specs=in_specs, out_specs=out_specs, check_vma=False)
```

```python
import jax
import jax.numpy as jnp
from jax import lax
from jax.experimental import pallas as pl
from jax.experimental.pallas import tpu as pltpu
from jax.sharding import PartitionSpec as P

MESH = pl.DeviceIdType.MESH
BF16, F32 = jnp.bfloat16, jnp.float32
LOG2E = 1.4426950408889634
LOWEST = -1e38
KEY_BLOCK = 256


class Copies:
    def __init__(self, send_sem, recv_sem):
        self.send_sem, self.recv_sem, self.used = send_sem, recv_sem, 0

    def take(self, count):
        first = self.used
        self.used += count
        return first

    def make(self, index, src, dst, device):
        return pltpu.make_async_remote_copy(
            src_ref=src, dst_ref=dst, send_sem=self.send_sem.at[index], recv_sem=self.recv_sem.at[index],
            device_id=device, device_id_type=MESH)


class RingGather:
    def __init__(self, copies, right_dev, left_dev, here, left, right, far, at_right, at_left, at_far):
        first = copies.take(6)
        self.own = {}
        self.got = {}
        for half in (0, 1):
            self.own['r', half] = copies.make(first + half, here(half), at_right(half), right_dev)
            self.own['l', half] = copies.make(first + 2 + half, here(half), at_left(half), left_dev)
            self.got['r', half] = copies.make(first + half, left(half), left(half), right_dev)
            self.got['l', half] = copies.make(first + 2 + half, right(half), right(half), left_dev)
        self.passed = (copies.make(first + 4, left(0), at_far(0), right_dev),
                       copies.make(first + 5, right(1), at_far(1), left_dev))
        self.far_got = (copies.make(first + 4, far(0), far(0), right_dev),
                        copies.make(first + 5, far(1), far(1), left_dev))

    def send(self):
        for key in (('r', 0), ('l', 1), ('r', 1), ('l', 0)):
            self.own[key].start()

    def relay(self):
        self.got['r', 0].wait_recv()
        self.passed[0].start()
        self.got['l', 1].wait_recv()
        self.passed[1].start()

    def near(self):
        self.got['r', 1].wait_recv()
        self.got['l', 0].wait_recv()

    def last(self):
        self.far_got[0].wait_recv()
        self.far_got[1].wait_recv()

    def drain(self):
        for copy in self.own.values():
            copy.wait_send()
        for copy in self.passed:
            copy.wait_send()


class ChipGather:
    def __init__(self, copies, right_dev, left_dev, sib_dev, region, own, left, right, far, other):
        def at(owner):
            return lambda half: region(owner, half)
        self.ring = RingGather(copies, right_dev, left_dev, at(own), at(left), at(right), at(far),
                               at(own), at(own), lambda half: region(left if half == 0 else right, half))
        self.out, self.back = {}, {}
        for name, owner in (('own', own), ('left', left), ('right', right), ('far', far)):
            for half in (0, 1):
                index = copies.take(1)
                self.out[name, half] = copies.make(index, region(owner, half), region(owner, half), sib_dev)
                self.back[name, half] = copies.make(index, region(other(owner), half), region(other(owner), half), sib_dev)

    def send(self):
        self.ring.send()
        self.out['own', 0].start()
        self.out['own', 1].start()

    def relay(self):
        self.ring.relay()
        self.out['left', 0].start()
        self.out['right', 1].start()

    def near(self):
        self.ring.near()
        self.out['left', 1].start()
        self.out['right', 0].start()

    def last(self):
        self.ring.last()
        self.out['far', 0].start()
        self.out['far', 1].start()

    def finish(self):
        for copy in self.back.values():
            copy.wait_recv()

    def drain(self):
        self.ring.drain()
        for copy in self.out.values():
            copy.wait_send()


def do_if(needed, action):
    if needed is None:
        action()
    else:
        pl.when(needed)(action)


class DirectGather:
    def __init__(self, copies, devs, sib_dev, region, owners, other, gives, takes):
        self.out, self.got, self.hand, self.back, self.gives, self.takes = {}, {}, {}, {}, gives, takes
        for name in ('left', 'right', 'far'):
            index = copies.take(1)
            self.out[name] = copies.make(index, region(owners['own']), region(owners['own']), devs[name])
            self.got[name] = copies.make(index, region(owners[name]), region(owners[name]), devs[name])
        for name, owner in owners.items():
            index = copies.take(1)
            self.hand[name] = copies.make(index, region(owner), region(owner), sib_dev)
            self.back[name] = copies.make(index, region(other(owner)), region(other(owner)), sib_dev)

    def send(self):
        for name, copy in self.out.items():
            do_if(self.gives[name], copy.start)
        self.hand['own'].start()

    def pass_on(self, name):
        def action():
            self.got[name].wait_recv()
            self.hand[name].start()
        do_if(self.takes[name], action)

    def near(self):
        self.pass_on('left')
        self.pass_on('right')

    def last(self):
        self.pass_on('far')

    def finish(self):
        for name in ('left', 'right', 'far'):
            do_if(self.takes[name], self.back[name].wait_recv)

    def drain(self):
        for name, copy in self.out.items():
            do_if(self.gives[name], copy.wait_send)
        for name, copy in self.hand.items():
            do_if(self.takes.get(name), copy.wait_send)


def layer_kernel(tp_size, cp_size, x_hbm, pos_hbm, gain_hbm, wq_hbm, wk_hbm, wv_hbm, wo_hbm, freq_hbm,
                 y_out, kv_out,
                 xv, hv, gain_raw, gain_v, pos_v, freq_v, wkv, wq, wo, kv, qs, cos_v, sin_v, cap_v, scores, run_max,
                 run_sum, acc, oall, load_sem, send_sem, recv_sem):
    rows, width = xv.shape
    piece = rows // 2
    head_dim = wk_hbm.shape[1]
    half_dim = head_dim // 2
    head_cols = wq_hbm.shape[1]
    heads = head_cols // head_dim
    out_cols = width // tp_size
    low_rows = piece * cp_size
    share = head_cols // cp_size
    cut = (share // 2 + 15) // 16 * 16
    score_scale = head_dim ** -0.5 * LOG2E

    t = lax.axis_index('tp')
    c = lax.axis_index('cp')
    chips = cp_size // 2
    core = lax.rem(c, 2)
    chip = c // 2

    def tp_at(step):
        return lax.rem(t + step, tp_size)

    def cp_at(step):
        return lax.rem(chip + step, chips) * 2 + core

    def other(owner):
        return owner + 1 - 2 * core

    up, down = {'tp': tp_at(1)}, {'tp': tp_at(tp_size - 1)}
    right, left, far, sib = {'cp': cp_at(1)}, {'cp': cp_at(chips - 1)}, {'cp': cp_at(2)}, {'cp': other(c)}

    loads = {}

    def load(name, src, dst):
        loads[name] = pltpu.make_async_copy(src, dst, load_sem.at[len(loads)])
        loads[name].start()

    load('pos', pos_hbm, pos_v)
    load('freq', freq_hbm, freq_v)
    load('gain', gain_hbm, gain_raw)
    load(('x', 0), x_hbm.at[pl.ds(0, piece)], xv.at[pl.ds(0, piece)])
    load('wk', wk_hbm, wkv.at[:, pl.ds(0, head_dim)])
    load('wv', wv_hbm, wkv.at[:, pl.ds(head_dim, head_dim)])
    load(('x', 1), x_hbm.at[pl.ds(piece, piece)], xv.at[pl.ds(piece, piece)])
    own_cols = pl.multiple_of(t * out_cols, 128)
    q_chunks = ((0, 4), (4, heads - 4))

    barrier = pltpu.get_barrier_semaphore()
    peers = [{'tp': tp_at(step)} for step in range(1, tp_size)] + [right, left, far, sib]
    for peer in peers:
        pl.semaphore_signal(barrier, inc=1, device_id=peer, device_id_type=MESH)

    copies = Copies(send_sem, recv_sem)

    col_chunks = ((0, 384), (384, 256), (640, out_cols - 640))
    share_row = pl.multiple_of(c * share, 16)
    wo_out, wo_in = {}, {}
    for n, (start, size) in enumerate(col_chunks):
        for step in range(1, tp_size):
            index = copies.take(1)
            src_col = pl.multiple_of(tp_at(step) * out_cols + start, 128)
            wo_out[n, step] = copies.make(
                index, wo_hbm.at[pl.ds(share_row, share), pl.ds(src_col, size)],
                wo.at[tp_size - step, pl.ds(share_row, share), pl.ds(start, size)], {'tp': tp_at(step)})
            landed = wo.at[tp_size - step, pl.ds(share_row, share), pl.ds(start, size)]
            wo_in[n, step] = copies.make(index, landed, landed, {'tp': tp_at(step)})

    def wo_region(n):
        start, size = col_chunks[n]

        def region(owner, half):
            first = pl.multiple_of(owner * share + (cut if half else 0), 16)
            return wo.at[pl.ds(1, tp_size - 1), pl.ds(first, share - cut if half else cut), pl.ds(start, size)]
        return region

    def kv_region(p, kind):
        def region(owner):
            return kv.at[kind, pl.ds(pl.multiple_of(p * low_rows + owner * piece, piece), piece)]
        return region

    def chip_gather(region):
        return ChipGather(copies, right, left, sib, region, c, cp_at(chips - 1), cp_at(1), cp_at(2), other)

    cp_devs = {'left': right, 'right': left, 'far': far}
    steps = {'left': chips - 1, 'right': 1, 'far': 2}
    owners = {'own': c, **{name: cp_at(step) for name, step in steps.items()}}
    always = dict.fromkeys(steps)
    gives = {name: lax.rem(chip + chips - step, chips) < chip for name, step in steps.items()}
    takes = {name: lax.rem(chip + step, chips) > chip for name, step in steps.items()}
    kv_gather = {(p, kind): DirectGather(copies, cp_devs, sib, kv_region(p, kind), owners, other,
                                         gives if p else always, takes if p else always)
                 for p in (0, 1) for kind in (0, 1)}
    wo_gather = [chip_gather(wo_region(n)) for n in range(len(col_chunks))]

    def o_gather_of(p):
        def at(slot):
            return lambda half: oall.at[slot, pl.ds(p * piece + half * (piece // 2), piece // 2)]
        return RingGather(copies, up, down, at(0), at(3), at(1), at(2), at(3), at(1), at(2))

    def y_gather_of(p, n):
        start, size = col_chunks[n]

        def at(step):
            cols = pl.ds(pl.multiple_of(tp_at(step) * out_cols + start, 128), size)
            return lambda half: y_out.at[pl.ds(p * piece + half * (piece // 2), piece // 2), cols]

        def passed(half):
            return at(3 if half == 0 else 1)(half)
        return RingGather(copies, up, down, at(0), at(3), at(1), at(2), at(0), at(0), passed)

    o_gather = [o_gather_of(p) for p in (0, 1)]
    y_gather = {(p, n): y_gather_of(p, n) for p in (0, 1) for n in range(len(col_chunks))}

    loads['pos'].wait()
    loads['freq'].wait()
    freq = jnp.concatenate([freq_v[...], freq_v[...]], axis=-1)
    lower = lax.broadcasted_iota(jnp.int32, (piece, head_dim), 1) < half_dim

    def pos_column(p):
        pos_row = pos_v[:, pl.ds(p * piece, piece)].astype(F32)
        return jnp.transpose(jnp.broadcast_to(pos_row, (piece, piece)))

    angle = jnp.where(lower, pos_column(0), pos_column(1)) * freq
    cosine, sine = jnp.cos(angle), jnp.sin(angle)
    cosine_turned, sine_turned = pltpu.roll(cosine, half_dim, 1), pltpu.roll(sine, half_dim, 1)
    cos_v[0] = jnp.where(lower, cosine, cosine_turned)
    cos_v[1] = jnp.where(lower, cosine_turned, cosine)
    sin_v[0] = jnp.where(lower, -sine, sine_turned)
    sin_v[1] = jnp.where(lower, -sine_turned, sine)

    def rope(vec, p):
        vec = vec.astype(F32)
        return (vec * cos_v[p] + pltpu.roll(vec, half_dim, 1) * sin_v[p]).astype(BF16)

    loads['gain'].wait()
    for tile in range(width // 128):
        gain_v[:, tile * 128:(tile + 1) * 128] = gain_raw[tile:tile + 1, :]

    norm_rows = 32
    for p in (0, 1):
        loads['x', p].wait()

        def norm_step(step, _, p=p):
            part = pl.ds(pl.multiple_of(p * piece + step * norm_rows, norm_rows), norm_rows)
            x_f32 = xv[part, :].astype(F32)
            inv_rms = lax.rsqrt(jnp.mean(x_f32 * x_f32, axis=-1, keepdims=True) + 1e-5)
            hv[part, :] = (x_f32 * inv_rms * gain_v[...]).astype(BF16)
            return 0
        lax.fori_loop(0, piece // norm_rows, norm_step, 0)
        if p == 0:
            loads['wk'].wait()
            loads['wv'].wait()
            for first, count in q_chunks:
                cols = pl.ds(first * head_dim, count * head_dim)
                load(('wq', first), wq_hbm.at[:, cols], wq.at[:, cols])
            pl.semaphore_wait(barrier, len(peers))
            for copy in wo_out.values():
                copy.start()
        block = jnp.dot(hv[pl.ds(p * piece, piece), :], wkv[...], preferred_element_type=F32).astype(BF16)
        k_new, v_new = rope(block[:, :head_dim], p), block[:, head_dim:]
        kv_region(p, 0)(c)[...] = k_new
        kv_gather[p, 0].send()
        kv_region(p, 1)(c)[...] = v_new
        kv_gather[p, 1].send()
        kv_out[0, pl.ds(p * piece, piece), :] = k_new
        kv_out[1, pl.ds(p * piece, piece), :] = v_new
    load('wo', wo_hbm.at[:, pl.ds(own_cols, out_cols)], wo.at[0])

    def queries(first, count):
        loads['wq', first].wait()
        new = jnp.dot(hv[...], wq[:, pl.ds(first * head_dim, count * head_dim)], preferred_element_type=F32).astype(BF16)
        for h in range(count):
            for p in (0, 1):
                qs[p, pl.ds((first + h) * piece, piece), :] = rope(
                    new[p * piece:(p + 1) * piece, h * head_dim:(h + 1) * head_dim], p)

    def key_rows(block):
        return pl.ds(pl.multiple_of(block * KEY_BLOCK, KEY_BLOCK), KEY_BLOCK)

    run_max[...] = jnp.full(run_max.shape, LOWEST, F32)
    run_sum[...] = jnp.zeros(run_sum.shape, F32)

    def score(p, blocks):
        piece_id = c if p == 0 else 2 * cp_size - 1 - c
        q_idx = (piece_id * piece).astype(F32) + lax.broadcasted_iota(jnp.int32, (piece, piece), 0).astype(F32)
        doc_start = q_idx - pos_column(p)
        lane = lax.broadcasted_iota(jnp.int32, (piece, piece), 1).astype(F32)
        for n, block in enumerate(blocks):
            for half in (0, 1):
                owner = block * 2 + half
                owner_piece = jnp.where(owner < cp_size, owner, 3 * cp_size - 1 - owner)
                key_idx = (owner_piece * piece).astype(F32) + lane
                seen = (key_idx >= doc_start) & (key_idx <= q_idx)
                cap_v[n, :, half * piece:(half + 1) * piece] = jnp.where(seen, jnp.inf, -jnp.inf)
        raw = [lax.dot_general(qs[p], kv[0, key_rows(block), :], (((1,), (1,)), ((), ())), preferred_element_type=F32)
               for block in blocks]
        for h in range(heads):
            mine = slice(h * piece, (h + 1) * piece)
            parts = []
            for n, block in enumerate(blocks):
                capped = jnp.minimum(raw[n][mine] * score_scale, cap_v[n])
                scores[block + p * chips, mine, :] = capped
                parts += [capped[:, :piece], capped[:, piece:]]
            before = run_max[p, mine, :]
            top = before
            for part in parts:
                top = jnp.maximum(top, part)
            run_max[p, mine, :] = top
            total = run_sum[p, mine, :] * jnp.exp2(before - top)
            for part in parts:
                total = total + jnp.exp2(part - top)
            run_sum[p, mine, :] = total

    def score_loop(p, count, block_of):
        def step(i, _):
            score(p, [block_of(i)])
            return 0
        lax.fori_loop(0, count, step, 0)

    def close_scores(p):
        for h in range(heads):
            mine = slice(h * piece, (h + 1) * piece)
            lane_max = run_max[p, mine, :]
            top = jnp.broadcast_to(jnp.max(lane_max, axis=-1, keepdims=True), (piece, piece))
            total = jnp.sum(run_sum[p, mine, :] * jnp.exp2(lane_max - top), axis=-1, keepdims=True)
            run_max[p, mine, :] = top + jnp.broadcast_to(jnp.log2(total), (piece, piece))

    def value_loop(p, count, block_of):
        acc[...] = jnp.zeros(acc.shape, F32)

        def step(i, _):
            block = block_of(i)
            shift = run_max[p]
            probs = jnp.concatenate([jnp.exp2(scores[block + p * chips, :, :piece] - shift).astype(BF16),
                                     jnp.exp2(scores[block + p * chips, :, piece:] - shift).astype(BF16)], axis=-1)
            acc[...] += jnp.dot(probs, kv[1, key_rows(block), :], preferred_element_type=F32)
            return 0
        lax.fori_loop(0, count, step, 0)

    def close_piece(p):
        for h in range(heads):
            oall[0, pl.ds(p * piece, piece), h * head_dim:(h + 1) * head_dim] = (
                acc[h * piece:(h + 1) * piece, :].astype(BF16))
        o_gather[p].send()

    def project(p, n):
        start, size = col_chunks[n]
        part = pl.ds(p * piece, piece)
        total = xv[part, pl.ds(pl.multiple_of(own_cols + start, 128), size)].astype(F32)
        mixed = jnp.dot(oall[0, part, :], wo[0, :, pl.ds(start, size)], preferred_element_type=F32)
        for slot in range(1, tp_size):
            mixed = mixed + jnp.dot(oall[slot, part, :], wo[slot, :, pl.ds(start, size)], preferred_element_type=F32)
        y_out[part, pl.ds(pl.multiple_of(own_cols + start, 128), size)] = (total + mixed).astype(BF16)

    def wo_send(n):
        for step in range(1, tp_size):
            wo_in[n, step].wait_recv()
        wo_gather[n].send()

    queries(*q_chunks[0])
    kv_gather[0, 0].near()
    queries(*q_chunks[1])
    kv_gather[0, 0].back['own'].wait_recv()
    score(0, [chip])
    kv_gather[0, 0].last()
    kv_gather[0, 1].near()
    score(1, [chip])
    kv_gather[1, 0].back['own'].wait_recv()
    score(1, [chips + chip])
    wo_send(0)
    kv_gather[0, 0].finish()
    score_loop(0, chip, lambda i: i)
    close_scores(0)
    kv_gather[0, 1].last()
    kv_gather[0, 1].back['own'].wait_recv()
    kv_gather[0, 1].finish()
    value_loop(0, chip + 1, lambda i: i)
    close_piece(0)
    kv_gather[1, 0].near()
    kv_gather[1, 0].last()
    score(1, [lax.rem(chip + i, chips) for i in range(1, chips)])
    wo_gather[0].relay()
    wo_send(1)
    kv_gather[1, 1].near()
    kv_gather[1, 0].finish()
    score_loop(1, chips - 1 - chip, lambda i: chips + chip + 1 + i)
    kv_gather[1, 1].last()
    close_scores(1)
    o_gather[0].relay()
    kv_gather[1, 1].back['own'].wait_recv()
    kv_gather[1, 1].finish()
    value_loop(1, 2 * chips - chip, lambda i: jnp.where(i < chips, i, i + chip))
    close_piece(1)

    o_gather[0].near()
    wo_gather[0].near()
    wo_gather[0].last()
    o_gather[0].last()
    wo_gather[1].relay()
    wo_send(2)
    loads['wo'].wait()
    wo_gather[0].finish()
    project(0, 0)
    o_gather[1].relay()
    y_gather[0, 0].send()
    wo_gather[1].near()
    wo_gather[1].last()
    wo_gather[1].finish()
    project(0, 1)
    y_gather[0, 1].send()
    wo_gather[2].relay()
    o_gather[1].near()
    o_gather[1].last()
    project(1, 0)
    y_gather[1, 0].send()
    project(1, 1)
    y_gather[1, 1].send()
    y_gather[0, 0].relay()
    wo_gather[2].near()
    y_gather[0, 1].relay()
    wo_gather[2].last()
    wo_gather[2].finish()
    project(0, 2)
    y_gather[0, 2].send()
    project(1, 2)
    y_gather[1, 2].send()
    y_gather[1, 0].relay()
    y_gather[1, 1].relay()
    y_gather[0, 2].relay()
    y_gather[1, 2].relay()
    for gather in y_gather.values():
        gather.near()
        gather.last()

    for copy in wo_out.values():
        copy.wait_send()
    for gather in list(kv_gather.values()) + wo_gather + o_gather + list(y_gather.values()):
        gather.drain()
    assert copies.used == send_sem.shape[0]


def solution(mesh):
    tp_size, cp_size = mesh.shape['tp'], mesh.shape['cp']

    def local_step(x_in, doc_id, pos_in_doc, norm_gain, w_q, w_k, w_v, w_o, inv_freq):
        del doc_id
        rows, width = x_in.shape
        piece = rows // 2
        head_dim = w_k.shape[1]
        head_cols = w_q.shape[1]
        heads = head_cols // head_dim
        out_cols = width // tp_size
        copies = 3 * (tp_size - 1) + 4 * 7 + 3 * 14 + 8 * 6
        stack = heads * piece
        y_out, kv_new = pl.pallas_call(
            lambda *refs: layer_kernel(tp_size, cp_size, *refs),
            out_shape=(jax.ShapeDtypeStruct(x_in.shape, BF16), jax.ShapeDtypeStruct((2, rows, head_dim), BF16)),
            in_specs=[pl.BlockSpec(memory_space=pltpu.HBM)] * 8,
            out_specs=[pl.BlockSpec(memory_space=pltpu.VMEM)] * 2,
            scratch_shapes=[
                pltpu.VMEM((rows, width), BF16),
                pltpu.VMEM((rows, width), BF16),
                pltpu.VMEM((width // 128, 128), F32),
                pltpu.VMEM((1, width), F32),
                pltpu.VMEM((1, rows), jnp.int32),
                pltpu.VMEM((1, head_dim // 2), F32),
                pltpu.VMEM((width, 2 * head_dim), BF16),
                pltpu.VMEM((width, head_cols), BF16),
                pltpu.VMEM((tp_size, head_cols, out_cols), BF16),
                pltpu.VMEM((2, rows * cp_size, head_dim), BF16),
                pltpu.VMEM((2, stack, head_dim), BF16),
                pltpu.VMEM((2, piece, head_dim), F32),
                pltpu.VMEM((2, piece, head_dim), F32),
                pltpu.VMEM((cp_size // 2 - 1, piece, KEY_BLOCK), F32),
                pltpu.VMEM((3 * cp_size // 2, stack, KEY_BLOCK), F32),
                pltpu.VMEM((2, stack, piece), F32),
                pltpu.VMEM((2, stack, piece), F32),
                pltpu.VMEM((stack, head_dim), F32),
                pltpu.VMEM((tp_size, rows, head_cols), BF16),
                pltpu.SemaphoreType.DMA((10,)),
                pltpu.SemaphoreType.DMA((copies,)),
                pltpu.SemaphoreType.DMA((copies,)),
            ],
            compiler_params=pltpu.CompilerParams(
                collective_id=0, has_side_effects=True, vmem_limit_bytes=44 * 1024 * 1024),
            name='layer',
        )(*[pltpu.with_memory_space_constraint(a, pltpu.HBM) for a in (
            x_in, pos_in_doc.reshape(1, rows), norm_gain.reshape(width // 128, 128), w_q, w_k, w_v, w_o,
            inv_freq.reshape(1, head_dim // 2))])
        kv_heads = 1
        return y_out, kv_new[0].reshape(rows, kv_heads, head_dim), kv_new[1].reshape(rows, kv_heads, head_dim)

    row_spec = P(('dp', 'cp'))
    in_specs = (P(('dp', 'cp'), None), row_spec, row_spec, P(), P(None, 'tp'), P(None, 'tp'), P(None, 'tp'), P('tp', None), P())
    out_specs = (P(('dp', 'cp'), None), P(('dp', 'cp'), 'tp', None), P(('dp', 'cp'), 'tp', None))
    return jax.shard_map(local_step, mesh=mesh, in_specs=in_specs, out_specs=out_specs, check_vma=False)
```
